32 devices in a mesh: dp: 1 (over z), ep: 32 (over y, x, core).
Axes of the slice: x: 4, y: 4, z: 1, core: 2. Of those that a mesh axis runs over, the one named last changes fastest.
The devices are a block of a 4x4x8 slice.
Arguments:
- x_in: bfloat16 [16384, 256], P(('dp', 'ep'))
- idx_a: int32 [16384, 8], P(('dp', 'ep'))
- idx_b: int32 [16384, 8], P(('dp', 'ep'))
- gate_a: float32 [16384, 8], P(('dp', 'ep'))
- gate_b: float32 [16384, 8], P(('dp', 'ep'))
- dy_out: bfloat16 [16384, 256], P(('dp', 'ep'))
- w1_a: bfloat16 [32, 256, 128], P('ep')
- w3_a: bfloat16 [32, 256, 128], P('ep')
- w2_a: bfloat16 [32, 128, 256], P('ep')
- w1_b: bfloat16 [32, 256, 128], P('ep')
- w3_b: bfloat16 [32, 256, 128], P('ep')
- w2_b: bfloat16 [32, 128, 256], P('ep')
Outputs:
- output 1: bfloat16 [16384, 256], P(('dp', 'ep'))
- output 2: bfloat16 [16384, 256], P(('dp', 'ep'))
- output 3: float32 [32, 256, 128], P(('dp', 'ep'))
- output 4: float32 [32, 256, 128], P(('dp', 'ep'))
- output 5: float32 [32, 128, 256], P(('dp', 'ep'))
- output 6: float32 [32, 256, 128], P(('dp', 'ep'))
- output 7: float32 [32, 256, 128], P(('dp', 'ep'))
- output 8: float32 [32, 128, 256], P(('dp', 'ep'))
- output 9: float32 [16384, 8], P(('dp', 'ep'))
- output 10: float32 [16384, 8], P(('dp', 'ep'))
All inputs are finite; a program needn't handle non-finite values.
Results may differ from the reference program's by a relative error of at most 0.005832.
Values are sent between devices in bfloat16 or wider.
A program may use at most 768 MiB of HBM per device.

```python
import jax
import jax.numpy as jnp
from jax import lax

TOKENS = 512
D = 256
FF = 128
EXPERTS = 32
TOP = 8
GROUP = 32
CAP = 512
HOT = 2


def draw_routing(root_key):
    key_hot, key_dev = jax.random.split(root_key)
    ranking = jax.random.permutation(key_hot, EXPERTS)
    cold_total = EXPERTS - HOT
    spare_pairs = TOKENS * TOP - HOT * CAP
    base_count = spare_pairs // cold_total
    extra_count = spare_pairs - base_count * cold_total

    def one_device(dev_key):
        key_count, key_rows, key_shift = jax.random.split(dev_key, 3)
        cold_rank = jax.random.permutation(key_count, cold_total)
        cold_count = base_count + (cold_rank < extra_count).astype(jnp.int32)
        by_rank = jnp.concatenate([jnp.full((HOT,), CAP, jnp.int32), cold_count])
        expert_count = jnp.zeros((EXPERTS,), jnp.int32).at[ranking].set(by_rank)
        run_ends = jnp.cumsum(expert_count)
        positions = jnp.arange(TOKENS * TOP, dtype=jnp.int32)
        sorted_ids = jnp.searchsorted(run_ends, positions, side="right").astype(jnp.int32)
        id_table = sorted_ids.reshape(TOP, TOKENS).T
        id_table = id_table[jax.random.permutation(key_rows, TOKENS)]
        row_shift = jax.random.randint(key_shift, (TOKENS, 1), 0, TOP)
        col_order = (jnp.arange(TOP)[None, :] + row_shift) % TOP
        return jnp.take_along_axis(id_table, col_order, axis=1)

    return jax.vmap(one_device)(jax.random.split(key_dev, GROUP)).reshape(GROUP * TOKENS, TOP)


def setup_inputs(seed: int = 0, part: int = 0) -> dict:
    root_key = jax.random.key(seed)
    shared_keys = jax.random.split(root_key, 6)
    part_keys = jax.random.split(jax.random.fold_in(root_key, part), 6)
    row_total = GROUP * TOKENS
    gate_scale = 1.5 / TOP ** 0.5
    in_scale = D ** -0.5
    mid_scale = FF ** -0.5
    x_in = jax.random.normal(part_keys[0], (row_total, D), jnp.float32).astype(jnp.bfloat16)
    idx_a = draw_routing(part_keys[1])
    idx_b = draw_routing(part_keys[2])
    gate_a = (0.5 + jax.random.uniform(part_keys[3], (row_total, TOP), jnp.float32)) * gate_scale
    gate_b = (0.5 + jax.random.uniform(part_keys[4], (row_total, TOP), jnp.float32)) * gate_scale
    dy_out = jax.random.normal(part_keys[5], (row_total, D), jnp.float32).astype(jnp.bfloat16)
    w1_a = (jax.random.normal(shared_keys[0], (EXPERTS, D, FF), jnp.float32) * in_scale).astype(jnp.bfloat16)
    w3_a = (jax.random.normal(shared_keys[1], (EXPERTS, D, FF), jnp.float32) * in_scale).astype(jnp.bfloat16)
    w2_a = (jax.random.normal(shared_keys[2], (EXPERTS, FF, D), jnp.float32) * mid_scale).astype(jnp.bfloat16)
    w1_b = (jax.random.normal(shared_keys[3], (EXPERTS, D, FF), jnp.float32) * in_scale).astype(jnp.bfloat16)
    w3_b = (jax.random.normal(shared_keys[4], (EXPERTS, D, FF), jnp.float32) * in_scale).astype(jnp.bfloat16)
    w2_b = (jax.random.normal(shared_keys[5], (EXPERTS, FF, D), jnp.float32) * mid_scale).astype(jnp.bfloat16)
    return {"x_in": x_in, "idx_a": idx_a, "idx_b": idx_b, "gate_a": gate_a, "gate_b": gate_b, "dy_out": dy_out, "w1_a": w1_a, "w3_a": w3_a, "w2_a": w2_a, "w1_b": w1_b, "w3_b": w3_b, "w2_b": w2_b}


def expert_forward(u_rows, w_gate, w_up, w_down):
    pre_gate = jnp.dot(u_rows, w_gate, preferred_element_type=jnp.float32)
    pre_up = jnp.dot(u_rows, w_up, preferred_element_type=jnp.float32)
    hidden = (jax.nn.silu(pre_gate) * pre_up).astype(jnp.bfloat16)
    out_rows = jnp.dot(hidden, w_down, preferred_element_type=jnp.float32).astype(jnp.bfloat16)
    return pre_gate, pre_up, hidden, out_rows


def device_slots(flat_ids):
    onehot = (flat_ids[:, None] == jnp.arange(EXPERTS, dtype=jnp.int32)[None, :]).astype(jnp.int32)
    return jnp.sum(jnp.cumsum(onehot, axis=0) * onehot, axis=1) - 1


def expert_table(ids):
    per_device = ids.reshape(GROUP, TOKENS * TOP)
    pair_slot = lax.map(device_slots, per_device)
    expert_row = jnp.arange(GROUP, dtype=jnp.int32)[:, None] * CAP + pair_slot
    pair_ids = jnp.arange(GROUP * TOKENS * TOP, dtype=jnp.int32).reshape(GROUP, TOKENS * TOP)
    empty_pair = GROUP * TOKENS * TOP
    return jnp.full((EXPERTS, GROUP * CAP), empty_pair, jnp.int32).at[per_device, expert_row].set(pair_ids)


def layer_forward(x_rows, gates, table, w_gate, w_up, w_down):
    x_pad = jnp.concatenate([x_rows, jnp.zeros((1, D), x_rows.dtype)])
    gate_pad = jnp.concatenate([gates.reshape(-1), jnp.zeros((1,), gates.dtype)])

    def expert_step(out_acc, step_in):
        pair_ids, gate_w, up_w, down_w = step_in
        tok_index = pair_ids // TOP
        out_rows = expert_forward(x_pad[tok_index], gate_w, up_w, down_w)[3]
        weighted = gate_pad[pair_ids][:, None] * out_rows.astype(jnp.float32)
        return out_acc.at[tok_index].add(weighted), None

    out_acc = jnp.zeros((GROUP * TOKENS + 1, D), jnp.float32)
    out_acc = lax.scan(expert_step, out_acc, (table, w_gate, w_up, w_down))[0]
    return (x_rows.astype(jnp.float32) + out_acc[:-1]).astype(jnp.bfloat16)


def layer_backward(dy_rows, x_rows, gates, table, w_gate, w_up, w_down):
    x_pad = jnp.concatenate([x_rows, jnp.zeros((1, D), x_rows.dtype)])
    dy_pad = jnp.concatenate([dy_rows, jnp.zeros((1, D), dy_rows.dtype)])
    gate_pad = jnp.concatenate([gates.reshape(-1), jnp.zeros((1,), gates.dtype)])

    def expert_step(carry_in, step_in):
        dx_acc, dgate_acc = carry_in
        pair_ids, gate_w, up_w, down_w = step_in
        tok_index = pair_ids // TOP
        u_rows = x_pad[tok_index]
        dy_exp = dy_pad[tok_index].astype(jnp.float32)
        pre_gate, pre_up, hidden, out_rows = expert_forward(u_rows, gate_w, up_w, down_w)
        dgate_rows = jnp.sum(dy_exp * out_rows.astype(jnp.float32), axis=1)
        d_out = (gate_pad[pair_ids][:, None] * dy_exp).astype(jnp.bfloat16)
        dw_down = jnp.dot(hidden.T, d_out, preferred_element_type=jnp.float32)
        d_hidden = jnp.dot(d_out, down_w.T, preferred_element_type=jnp.float32)
        gate_sig = jax.nn.sigmoid(pre_gate)
        d_pre_gate = (d_hidden * pre_up * gate_sig * (1.0 + pre_gate * (1.0 - gate_sig))).astype(jnp.bfloat16)
        d_pre_up = (d_hidden * jax.nn.silu(pre_gate)).astype(jnp.bfloat16)
        dw_gate = jnp.dot(u_rows.T, d_pre_gate, preferred_element_type=jnp.float32)
        dw_up = jnp.dot(u_rows.T, d_pre_up, preferred_element_type=jnp.float32)
        du_rows = (jnp.dot(d_pre_gate, gate_w.T, preferred_element_type=jnp.float32) + jnp.dot(d_pre_up, up_w.T, preferred_element_type=jnp.float32)).astype(jnp.bfloat16)
        dx_acc = dx_acc.at[tok_index].add(du_rows.astype(jnp.float32))
        dgate_acc = dgate_acc.at[pair_ids].set(dgate_rows)
        return (dx_acc, dgate_acc), (dw_gate, dw_up, dw_down)

    dx_acc = jnp.zeros((GROUP * TOKENS + 1, D), jnp.float32)
    dgate_acc = jnp.zeros((GROUP * TOKENS * TOP + 1,), jnp.float32)
    (dx_acc, dgate_acc), grads = lax.scan(expert_step, (dx_acc, dgate_acc), (table, w_gate, w_up, w_down))
    dx_rows = (dy_rows.astype(jnp.float32) + dx_acc[:-1]).astype(jnp.bfloat16)
    return dx_rows, dgate_acc[:-1].reshape(GROUP * TOKENS, TOP), grads


def reference(x_in, idx_a, idx_b, gate_a, gate_b, dy_out, w1_a, w3_a, w2_a, w1_b, w3_b, w2_b):
    table_a = expert_table(idx_a)
    table_b = expert_table(idx_b)
    x_mid = layer_forward(x_in, gate_a, table_a, w1_a, w3_a, w2_a)
    x_out = layer_forward(x_mid, gate_b, table_b, w1_b, w3_b, w2_b)
    dx_mid, dgate_b, grads_b = layer_backward(dy_out, x_mid, gate_b, table_b, w1_b, w3_b, w2_b)
    dx_in, dgate_a, grads_a = layer_backward(dx_mid, x_in, gate_a, table_a, w1_a, w3_a, w2_a)
    return (x_out, dx_in, grads_a[0], grads_a[1], grads_a[2], grads_b[0], grads_b[1], grads_b[2], dgate_a, dgate_b)
```

```python
import functools

import jax
import jax.numpy as jnp
from jax import lax
from jax.experimental import pallas as pl
from jax.experimental.pallas import tpu as pltpu
from jax.sharding import PartitionSpec as P

F32 = jnp.float32
BF16 = jnp.bfloat16


def mm(a, b, ca, cb):
    return lax.dot_general(a, b, (((ca,), (cb,)), ((), ())), preferred_element_type=F32)


def route(expert, idx_t, gate_t):
    picked = idx_t == expert
    gate = jnp.sum(jnp.where(picked, gate_t, 0.0), axis=0, keepdims=True)
    count = jnp.sum(jnp.where(picked, 1.0, 0.0), axis=0, keepdims=True)
    return picked, gate, count > 0.5


def expert_in(w, x_t, mask):
    d = x_t.shape[0]
    ab = mm(jnp.concatenate([w[:d], w[d : 2 * d]], axis=1), x_t, 0, 0)
    ab = jnp.where(mask, ab, 0.0)
    f = w.shape[1]
    return ab[:f], ab[f:]


def down(w, d):
    return jnp.concatenate([w[2 * d : 2 * d + d // 2], w[2 * d + d // 2 :]], axis=1)


def expert_forward(w, x_t, mask):
    d = x_t.shape[0]
    a, b = expert_in(w, x_t, mask)
    s = jax.nn.sigmoid(a)
    silu = a * s
    h = (silu * b).astype(BF16)
    o = mm(down(w, d), h, 0, 0).astype(BF16)
    return a, b, s, silu, h, o


def expert_backward(w, x, dy_t, gate, a, b, s, silu, h, o):
    d = x.shape[1]
    dy = dy_t.astype(F32)
    dgate = jnp.sum(dy * o.astype(F32), axis=0, keepdims=True)
    q = (gate * dy).astype(BF16)
    dh = mm(down(w, d), q, 1, 0)
    dw2 = mm(h, q, 1, 1)
    da = (dh * b * s * (1.0 + a * (1.0 - s))).astype(BF16)
    db = (dh * silu).astype(BF16)
    dab = jnp.concatenate([da, db], axis=0)
    dw13_t = mm(dab, x, 1, 0)
    du = mm(jnp.concatenate([w[:d], w[d : 2 * d]], axis=1), dab, 1, 0).astype(BF16)
    return dgate, dw13_t, dw2, du


def forward_kernel(x_ref, idx_ref, gate_ref, w_ref, y_ref, xt_s, acc_s):
    xt_s[...] = x_ref[...].T
    acc_s[...] = xt_s[...].astype(F32)

    def body(e, carry):
        picked, gate, mask = route(e, idx_ref[...], gate_ref[...])
        o = expert_forward(w_ref[e], xt_s[...], mask)[5]
        acc_s[...] += gate * o.astype(F32)
        return carry

    lax.fori_loop(0, w_ref.shape[0], body, 0)
    y_ref[...] = acc_s[...].astype(BF16).T


def both_kernel(fwd, x_ref, dy_ref, idx_ref, gate_ref, w_ref, *refs):
    if fwd:
        y_ref, dx_ref, dg_ref, dw_ref, xt_s, dyt_s, dx_s, acc_s = refs
    else:
        dx_ref, dg_ref, dw_ref, xt_s, dyt_s, dx_s = refs
    d = x_ref.shape[1]
    xt_s[...] = x_ref[...].T
    dyt_s[...] = dy_ref[...].T
    dx_s[...] = dyt_s[...].astype(F32)
    if fwd:
        acc_s[...] = xt_s[...].astype(F32)
    dg_ref[...] = jnp.zeros_like(dg_ref)

    def body(e, carry):
        picked, gate, mask = route(e, idx_ref[...], gate_ref[...])
        parts = expert_forward(w_ref[e], xt_s[...], mask)
        if fwd:
            acc_s[...] += gate * parts[5].astype(F32)
        dgate, dw13_t, dw2, du = expert_backward(w_ref[e], x_ref[...], dyt_s[...], gate, *parts)
        dg_ref[...] += jnp.where(picked, dgate, 0.0)
        dw_ref[e, : 2 * w_ref.shape[2]] = dw13_t
        dw_ref[e, 2 * w_ref.shape[2] :] = dw2
        dx_s[...] += du.astype(F32)
        return carry

    lax.fori_loop(0, w_ref.shape[0], body, 0)
    dx_ref[...] = dx_s[...].astype(BF16).T
    if fwd:
        y_ref[...] = acc_s[...].astype(BF16).T


def call(kernel, outs, scratch, *args):
    vmem = pl.BlockSpec(memory_space=pltpu.VMEM)
    return pl.pallas_call(
        kernel,
        out_shape=outs,
        in_specs=[vmem] * len(args),
        out_specs=jax.tree.map(lambda _: vmem, outs),
        scratch_shapes=scratch,
        compiler_params=pltpu.CompilerParams(vmem_limit_bytes=48 * 2**20),
    )(*args)


def pack(w1, w3, w2):
    half = w2.shape[2] // 2
    return jnp.concatenate([w1[0], w3[0], w2[0, :, :half], w2[0, :, half:]], axis=0)


def unpack(dw, f):
    return dw[:, :f].transpose(0, 2, 1), dw[:, f : 2 * f].transpose(0, 2, 1), dw[:, 2 * f :]


def solution(mesh):
    tok_spec = P(("dp", "ep"))
    w_spec = P("ep")

    def device_program(x_in, idx_a, idx_b, gate_a, gate_b, dy_out, w1_a, w3_a, w2_a, w1_b, w3_b, w2_b):
        (tok, d), f = x_in.shape, w1_a.shape[2]
        w_a = lax.all_gather(pack(w1_a, w3_a, w2_a), "ep")
        w_b = lax.all_gather(pack(w1_b, w3_b, w2_b), "ep")
        n = w_a.shape[0]
        rows = jax.ShapeDtypeStruct((tok, d), BF16)
        dgs = jax.ShapeDtypeStruct((idx_a.shape[1], tok), F32)
        dws = jax.ShapeDtypeStruct((n, 2 * f + f, d), F32)
        xt, acc = pltpu.VMEM((d, tok), BF16), pltpu.VMEM((d, tok), F32)
        x_mid = call(forward_kernel, rows, [xt, acc], x_in, idx_a.T, gate_a.T, w_a)
        x_out, dx_mid, dg_b, dw_b = call(
            functools.partial(both_kernel, True), (rows, rows, dgs, dws), [xt, xt, acc, acc],
            x_mid, dy_out, idx_b.T, gate_b.T, w_b)
        dx_in, dg_a, dw_a = call(
            functools.partial(both_kernel, False), (rows, dgs, dws), [xt, xt, acc],
            x_in, dx_mid, idx_a.T, gate_a.T, w_a)
        dw_b = lax.psum_scatter(dw_b, "ep", scatter_dimension=0, tiled=True)
        dw_a = lax.psum_scatter(dw_a, "ep", scatter_dimension=0, tiled=True)
        return (x_out, dx_in) + unpack(dw_a, f) + unpack(dw_b, f) + (dg_a.T, dg_b.T)

    return jax.shard_map(device_program, mesh=mesh, in_specs=(tok_spec,) * 6 + (w_spec,) * 6, out_specs=(tok_spec,) * 10, check_vma=False)
```

```python
import functools
import math

import jax
import jax.numpy as jnp
from jax import lax
from jax.experimental import pallas as pl
from jax.experimental.pallas import tpu as pltpu
from jax.sharding import PartitionSpec as P

F32 = jnp.float32
BF16 = jnp.bfloat16
MESH = pl.DeviceIdType.MESH


def mm(a, b, ca, cb):
    return lax.dot_general(a, b, (((ca,), (cb,)), ((), ())), preferred_element_type=F32)


def route(expert, idx_t, gate_t):
    picked = idx_t == expert
    gate = jnp.sum(jnp.where(picked, gate_t, 0.0), axis=0, keepdims=True)
    count = jnp.sum(jnp.where(picked, 1.0, 0.0), axis=0, keepdims=True)
    return picked, gate, count > 0.5


def expert_in(w, x_t, mask):
    d = x_t.shape[0]
    ab = mm(jnp.concatenate([w[:d], w[d : 2 * d]], axis=1), x_t, 0, 0)
    ab = jnp.where(mask, ab, 0.0)
    f = w.shape[1]
    return ab[:f], ab[f:]


def down(w, d):
    return jnp.concatenate([w[2 * d : 2 * d + d // 2], w[2 * d + d // 2 :]], axis=1)


def expert_forward(w, x_t, mask):
    d = x_t.shape[0]
    a, b = expert_in(w, x_t, mask)
    s = jax.nn.sigmoid(a)
    silu = a * s
    h = (silu * b).astype(BF16)
    o = mm(down(w, d), h, 0, 0).astype(BF16)
    return a, b, s, silu, h, o


def expert_backward(w, x, dy_t, gate, a, b, s, silu, h, o):
    d = x.shape[1]
    dy = dy_t.astype(F32)
    dgate = jnp.sum(dy * o.astype(F32), axis=0, keepdims=True)
    q = (gate * dy).astype(BF16)
    dh = mm(down(w, d), q, 1, 0)
    dw2 = mm(h, q, 1, 1)
    da = (dh * b * s * (1.0 + a * (1.0 - s))).astype(BF16)
    db = (dh * silu).astype(BF16)
    dab = jnp.concatenate([da, db], axis=0)
    dw13_t = mm(dab, x, 1, 0)
    du = mm(jnp.concatenate([w[:d], w[d : 2 * d]], axis=1), dab, 1, 0).astype(BF16)
    return dgate, dw13_t, dw2, du


def near_order(g):
    return g + lax.div(g, 2) * (1 - 2 * lax.rem(g, 2))


def far_order(g):
    return 2 - g + lax.div(g, 2) * (3 - 2 * lax.rem(g, 2))


def step_kernel(side, x_ref, dy_ref, ia_ref, ib_ref, ga_ref, gb_ref, w1a, w3a, w2a, w1b, w3b, w2b,
                xo_ref, dxi_ref, dw1a, dw3a, dw2a, dw1b, dw3b, dw2b, dga_ref, dgb_ref,
                wb, dwo, dws, rb, ah, af, bh, bf, xt, xm, xmt, dyt, acc, dxs,
                load_sem, ag_send, ag_recv, ag_pair, d_send, d_recv, pa_send, ah_recv, af_recv, pb_send, bh_recv, bf_recv):
    me = lax.axis_index("ep")
    core, chip = lax.rem(me, 2), lax.div(me, 2)
    cx, cy = lax.rem(chip, side), lax.div(chip, side)
    p = cx * (1 - core) + cy * core
    r = cy * (1 - core) + cx * core
    tok, d = x_ref.shape
    f = w1a.shape[2]
    wrows, grows = wb.shape[2], dwo.shape[2]
    wh, gh = wrows // 2, grows // 2
    steps = side * side
    ring = dws.shape[0]

    def member(i, j, c):
        return ((j * (1 - c) + i * c) * side + i * (1 - c) + j * c) * 2 + c

    def at(di, dj):
        return member(lax.rem(p + di, side), lax.rem(r + dj, side), core)

    sib = me + 1 - 2 * core
    first = {1: at(1, 0), -1: at(side - 1, 0)}
    second = {1: at(0, 1), -1: at(0, side - 1)}

    def rdma(src, dst, send, recv, dev):
        return pltpu.make_async_remote_copy(src_ref=src, dst_ref=dst, send_sem=send, recv_sem=recv, device_id={"ep": dev}, device_id_type=MESH)

    loads = []
    for layer, (w1, w3, w2) in enumerate(((w1a, w3a, w2a), (w1b, w3b, w2b))):
        parts = (w1.at[0], w3.at[0], w2.at[0, :, pl.ds(0, d // 2)], w2.at[0, :, pl.ds(d // 2, d // 2)])
        row = 0
        for n, part in enumerate(parts):
            loads.append(pltpu.make_async_copy(part, wb.at[layer, me, pl.ds(row, part.shape[0])], load_sem.at[4 * layer + n]))
            row += part.shape[0]
    for copy in loads:
        copy.start()

    barrier = pltpu.get_barrier_semaphore()
    for dev in (sib, *first.values(), *second.values()):
        pl.semaphore_signal(barrier, inc=1, device_id={"ep": dev}, device_id_type=MESH)
    pl.semaphore_wait(barrier, 5)

    ag_slots = []

    def ag_copy(layer, e, half, dev, pair=False):
        view = wb.at[layer, e] if half is None else wb.at[layer, e, pl.ds(half * wh, wh)]
        recv = ag_pair.at[layer, e] if pair else ag_recv.at[layer, e, half or 0]
        copy = rdma(view, view, ag_send.at[len(ag_slots)], recv, dev)
        ag_slots.append(half)
        copy.start()

    def ag_wait(layer, e, half):
        view = wb.at[layer, e] if half is None else wb.at[layer, e, pl.ds(half * wh, wh)]
        rdma(view, view, ag_send.at[0], ag_recv.at[layer, e, half or 0], me).wait_recv()

    def spread(layer, di):
        for dev in second.values():
            ag_copy(layer, at(di, 0), None, dev)

    def arrive(layer, di, dj):
        e = at(di, dj)
        last = dj or di
        if last == 2:
            ag_wait(layer, e, 0)
            ag_wait(layer, e, 1)
        elif last:
            ag_wait(layer, e, None)
        line = second if dj else first
        if last == 3:
            ag_copy(layer, e, 0, line[1])
        if last == 1:
            ag_copy(layer, e, 1, line[-1])
        ag_copy(layer, e, None, sib, pair=True)

    def own_out(layer):
        for dev in first.values():
            ag_copy(layer, me, None, dev)

    def pair_wait(layer, e):
        view = wb.at[layer, e]
        rdma(view, view, ag_send.at[0], ag_pair.at[layer, e], me).wait_recv()

    for copy in loads[:4]:
        copy.wait()
    own_out(0)
    spread(0, 0)
    arrive(0, 0, 0)
    xt[...] = x_ref[...].T
    dyt[...] = dy_ref[...].T
    acc[...] = xt[...].astype(F32)
    dxs[...] = dyt[...].astype(F32)
    dga_ref[...] = jnp.zeros_like(dga_ref)
    dgb_ref[...] = jnp.zeros_like(dgb_ref)
    for copy in loads[4:]:
        copy.wait()

    def actions(k, table):
        for step, todo in table.items():
            @pl.when(k == step)
            def _():
                for fn, *args in todo:
                    fn(*args)

    def pick(order, k):
        a, b = order(lax.div(k, side)), order(lax.rem(k, side))
        return at(a, b), member(lax.rem(r + a, side), lax.rem(p + b, side), 1 - core)

    def forward_one(e):
        _, gate, mask = route(e, ia_ref[...], ga_ref[...])
        o = expert_forward(wb[0, e], xt[...], mask)[5]
        acc[...] += gate * o.astype(F32)

    first_pass = {
        1: [(arrive, 0, 1, 0), (arrive, 0, 3, 0), (arrive, 0, 0, 1), (arrive, 0, 0, 3), (spread, 0, 1), (spread, 0, 3)],
        3: [(arrive, 0, 0, 2), (arrive, 0, 2, 0), (spread, 0, 2)],
        4: [(arrive, 0, 1, 1), (arrive, 0, 1, 3)],
        6: [(own_out, 1), (arrive, 1, 0, 0)],
        7: [(arrive, 0, 1, 2)],
        8: [(arrive, 0, 3, 1), (arrive, 0, 3, 3)],
        9: [(arrive, 1, 1, 0), (arrive, 1, 3, 0)],
        11: [(arrive, 0, 3, 2)],
        12: [(arrive, 0, 2, 1), (arrive, 0, 2, 3), (arrive, 1, 2, 0), (spread, 1, 2)],
        15: [(arrive, 0, 2, 2), (arrive, 1, 2, 1), (arrive, 1, 2, 3), (spread, 1, 1)],
    }
    second_pass = {
        0: [(arrive, 1, 2, 2)],
        2: [(spread, 1, 3)],
        3: [(arrive, 1, 1, 1), (arrive, 1, 1, 3)],
        4: [(arrive, 1, 1, 2)],
        6: [(spread, 1, 0)],
        7: [(arrive, 1, 3, 1), (arrive, 1, 3, 3)],
        8: [(arrive, 1, 3, 2)],
        11: [(arrive, 1, 0, 1), (arrive, 1, 0, 3)],
        12: [(arrive, 1, 0, 2)],
    }

    def forward_body(k, carry):
        actions(k, first_pass)
        own, other = pick(near_order, k)
        forward_one(own)
        pair_wait(0, other)
        forward_one(other)
        return carry

    lax.fori_loop(0, steps, forward_body, 0)
    xmt[...] = acc[...].astype(BF16)
    xm[...] = xmt[...].T
    acc[...] = xmt[...].astype(F32)

    def pair_send(layer, k):
        slot = lax.rem(k, ring)
        return rdma(dws.at[slot], rb.at[layer, k], d_send.at[slot], d_recv.at[layer, k], sib)

    def join(layer, k):
        pair_send(layer, k).wait_recv()
        dwo[layer, k] += rb[layer, k]

    lo, hi = pl.ds(0, gh), pl.ds(gh, gh)

    def far_copies(layer, g):
        return (rdma(dwo.at[layer, 4 * g, lo], ah.at[layer, g, 0], pa_send.at[layer, g, 0], ah_recv.at[layer, g, 0], second[1]),
                rdma(dwo.at[layer, 4 * g, hi], ah.at[layer, g, 1], pa_send.at[layer, g, 1], ah_recv.at[layer, g, 1], second[-1]))

    def near_copies(layer, g):
        return (rdma(dwo.at[layer, 4 * g + 1, hi], af.at[layer, g, 0, hi], pa_send.at[layer, g, 2], af_recv.at[layer, g, 0], second[1]),
                rdma(dwo.at[layer, 4 * g + 1, lo], af.at[layer, g, 0, lo], pa_send.at[layer, g, 3], af_recv.at[layer, g, 1], second[1]),
                rdma(dwo.at[layer, 4 * g + 2], af.at[layer, g, 1], pa_send.at[layer, g, 4], af_recv.at[layer, g, 2], second[-1]))

    def line_far(layer):
        return (rdma(dwo.at[layer, 3, lo], bh.at[layer, 0], pb_send.at[layer, 0], bh_recv.at[layer, 0], first[1]),
                rdma(dwo.at[layer, 3, hi], bh.at[layer, 1], pb_send.at[layer, 1], bh_recv.at[layer, 1], first[-1]))

    def line_near(layer):
        return (rdma(dwo.at[layer, 7], bf.at[layer, 0], pb_send.at[layer, 2], bf_recv.at[layer, 0], first[1]),
                rdma(dwo.at[layer, 11], bf.at[layer, 1], pb_send.at[layer, 3], bf_recv.at[layer, 1], first[-1]))

    def add_far(layer, g):
        for n, copy in enumerate(far_copies(layer, g)):
            copy.wait_recv()
            part = pl.ds(n * gh, gh)
            dwo[layer, 4 * g + 1 + n, part] += ah[layer, g, n]

    def add_near(layer, g):
        for copy in near_copies(layer, g):
            copy.wait_recv()
        dwo[layer, 4 * g + 3] += af[layer, g, 0] + af[layer, g, 1]

    def add_line(layer, n):
        line_far(layer)[n].wait_recv()
        part = pl.ds(n * gh, gh)
        dwo[layer, 7 + 4 * n, part] += bh[layer, n]

    def finish(layer, dw1, dw3, dw2):
        add_near(layer, 3)
        for copy in line_near(layer):
            copy.wait_recv()
        total = dwo[layer, 15] + bf[layer, 0] + bf[layer, 1]
        dw1[0] = total[:f].T
        dw3[0] = total[f : 2 * f].T
        dw2[0] = total[2 * f :]

    def middle(layer, k):
        g, part = lax.div(k, 4), lax.rem(k, 4)

        @pl.when(k >= 1)
        def _():
            join(layer, k - 1)

        @pl.when(part == 3)
        def _():
            add_far(layer, g)

        @pl.when((part == 2) & (k >= 6))
        def _():
            add_near(layer, g - 1)

        @pl.when(k == 10)
        def _():
            add_line(layer, 0)

        @pl.when(k == 14)
        def _():
            add_line(layer, 1)

    def end(layer, k):
        g, part = lax.div(k, 4), lax.rem(k, 4)

        @pl.when(part == 1)
        def _():
            for copy in far_copies(layer, g):
                copy.start()

        @pl.when(part == 2)
        def _():
            near_copies(layer, g)[0].start()

        @pl.when(part == 3)
        def _():
            for copy in near_copies(layer, g)[1:]:
                copy.start()

        @pl.when(k == 6)
        def _():
            for copy in line_far(layer):
                copy.start()

        @pl.when(k == 10)
        def _():
            line_near(layer)[0].start()

        @pl.when(k == 14)
        def _():
            line_near(layer)[1].start()

    def backward_one(layer, e, dst):
        idx, gates, dg = ((ia_ref, ga_ref, dga_ref), (ib_ref, gb_ref, dgb_ref))[layer]
        feat, rows = ((xt, x_ref), (xmt, xm))[layer]
        picked, gate, mask = route(e, idx[...], gates[...])
        w = wb[layer, e]
        parts = expert_forward(w, feat[...], mask)
        if layer:
            acc[...] += gate * parts[5].astype(F32)
        dgate, dw13_t, dw2, du = expert_backward(w, rows[...], dyt[...], gate, *parts)
        dg[...] += jnp.where(picked, dgate, 0.0)
        dst[: 2 * f] = dw13_t
        dst[2 * f :] = dw2
        dxs[...] += du.astype(F32)

    def backward_body(layer, k, carry):
        own, other = pick(far_order, k)
        if layer:
            actions(k, second_pass)
            pair_wait(1, other)

            @pl.when(k >= ring)
            def _():
                pair_send(layer, k).wait_send()
        else:
            pair_send(layer, k).wait_send()
        backward_one(layer, other, dws.at[lax.rem(k, ring)])
        middle(layer, k)
        if not layer:
            @pl.when(k == 0)
            def _():
                join(1, steps - 1)

            @pl.when(k == 3)
            def _():
                finish(1, dw1b, dw3b, dw2b)
        pair_send(layer, k).start()
        backward_one(layer, own, dwo.at[layer, k])
        end(layer, k)
        return carry

    lax.fori_loop(0, steps, functools.partial(backward_body, 1), 0)
    dyt[...] = dxs[...].astype(BF16)
    dxs[...] = dyt[...].astype(F32)
    xo_ref[...] = acc[...].astype(BF16).T
    lax.fori_loop(0, steps, functools.partial(backward_body, 0), 0)
    dxi_ref[...] = dxs[...].astype(BF16).T
    join(0, steps - 1)
    finish(0, dw1a, dw3a, dw2a)

    for n, half in enumerate(ag_slots):
        view = wb.at[0, 0] if half is None else wb.at[0, 0, pl.ds(0, wh)]
        rdma(view, view, ag_send.at[n], ag_recv.at[0, 0, 0], me).wait_send()
    for k in range(steps - ring, steps):
        pair_send(0, k).wait_send()
    for layer in range(2):
        for g in range(side):
            for copy in far_copies(layer, g) + near_copies(layer, g):
                copy.wait_send()
        for copy in line_far(layer) + line_near(layer):
            copy.wait_send()


def solution(mesh):
    tok_spec = P(("dp", "ep"))
    w_spec = P("ep")
    members = mesh.shape["ep"]
    side = math.isqrt(members // 2)
    chips = side * side

    def device_program(x_in, idx_a, idx_b, gate_a, gate_b, dy_out, w1_a, w3_a, w2_a, w1_b, w3_b, w2_b):
        (tok, d), top, f = x_in.shape, idx_a.shape[1], w1_a.shape[2]
        vmem, any_ = pl.BlockSpec(memory_space=pltpu.VMEM), pl.BlockSpec(memory_space=pl.ANY)
        shape = jax.ShapeDtypeStruct
        rows, dgs = shape((tok, d), BF16), shape((top, tok), F32)
        dws = (shape((1, d, f), F32), shape((1, d, f), F32), shape((1, f, d), F32))
        wrows, grows = 2 * d + 2 * f, 3 * f
        outs = pl.pallas_call(
            functools.partial(step_kernel, side),
            out_shape=(rows, rows) + dws + dws + (dgs, dgs),
            in_specs=[vmem] * 6 + [any_] * 6,
            out_specs=(vmem,) * 10,
            scratch_shapes=[
                pltpu.VMEM((2, members, wrows, f), BF16),
                pltpu.VMEM((2, chips, grows, d), F32),
                pltpu.VMEM((4, grows, d), F32),
                pltpu.VMEM((2, chips, grows, d), F32),
                pltpu.VMEM((2, side, 2, grows // 2, d), F32),
                pltpu.VMEM((2, side, 2, grows, d), F32),
                pltpu.VMEM((2, 2, grows // 2, d), F32),
                pltpu.VMEM((2, 2, grows, d), F32),
                pltpu.VMEM((d, tok), BF16),
                pltpu.VMEM((tok, d), BF16),
                pltpu.VMEM((d, tok), BF16),
                pltpu.VMEM((d, tok), BF16),
                pltpu.VMEM((d, tok), F32),
                pltpu.VMEM((d, tok), F32),
                pltpu.SemaphoreType.DMA((8,)),
                pltpu.SemaphoreType.DMA((72,)),
                pltpu.SemaphoreType.DMA((2, members, 2)),
                pltpu.SemaphoreType.DMA((2, members)),
                pltpu.SemaphoreType.DMA((4,)),
                pltpu.SemaphoreType.DMA((2, chips)),
                pltpu.SemaphoreType.DMA((2, side, 5)),
                pltpu.SemaphoreType.DMA((2, side, 2)),
                pltpu.SemaphoreType.DMA((2, side, 3)),
                pltpu.SemaphoreType.DMA((2, 4)),
                pltpu.SemaphoreType.DMA((2, 2)),
                pltpu.SemaphoreType.DMA((2, 2)),
            ],
            compiler_params=pltpu.CompilerParams(collective_id=0, has_side_effects=True, vmem_limit_bytes=62 * 2**20),
        )(x_in, dy_out, idx_a.T, idx_b.T, gate_a.T, gate_b.T, w1_a, w3_a, w2_a, w1_b, w3_b, w2_b)
        return outs[:8] + (outs[8].T, outs[9].T)

    return jax.shard_map(device_program, mesh=mesh, in_specs=(tok_spec,) * 6 + (w_spec,) * 6, out_specs=(tok_spec,) * 10, check_vma=False)
```

```python
import functools
import math

import jax
import jax.numpy as jnp
from jax import lax
from jax.experimental import pallas as pl
from jax.experimental.pallas import tpu as pltpu
from jax.sharding import PartitionSpec as P

F32 = jnp.float32
BF16 = jnp.bfloat16
MESH = pl.DeviceIdType.MESH

PLAN = {
    0: [("own_out", 1), ("spread", 0, 0), ("arrive", 0, 1, 0), ("arrive", 0, 3, 0), ("spread", 0, 1), ("arrive", 0, 0, 3)],
    1: [("arrive", 1, 1, 0), ("arrive", 1, 3, 0)],
    2: [("arrive", 0, 0, 1)],
    3: [("spread", 0, 3)],
    4: [("arrive", 0, 2, 0), ("spread", 0, 2)],
    6: [("arrive", 0, 1, 3), ("arrive", 0, 0, 2)],
    7: [("arrive", 0, 1, 1), ("arrive", 1, 2, 0)],
    8: [("spread", 1, 2)],
    9: [("arrive", 0, 3, 3)],
    11: [("arrive", 0, 3, 1)],
    12: [("arrive", 0, 2, 1)],
    14: [("arrive", 0, 1, 2), ("arrive", 0, 2, 3)],
    18: [("arrive", 1, 2, 3), ("arrive", 1, 2, 1)],
    20: [("arrive", 0, 3, 2)],
    21: [("spread", 1, 1)],
    24: [("spread", 1, 0), ("spread", 1, 3)],
    27: [("arrive", 0, 2, 2)],
    28: [("arrive", 1, 2, 2)],
    29: [("arrive", 1, 0, 0)],
    33: [("arrive", 1, 1, 3), ("arrive", 1, 1, 1)],
    34: [("arrive", 1, 0, 1)],
    35: [("arrive", 1, 0, 3)],
    37: [("arrive", 1, 3, 1)],
    38: [("arrive", 1, 1, 2)],
    39: [("arrive", 1, 3, 3)],
    45: [("arrive", 1, 3, 2)],
    48: [("arrive", 1, 0, 2)],
}
SUMS = (
    {"far": 1, "near_up": 3, "near_down": 3, "join": 6, "line": 16, "last": 27},
    {"far": 1, "near_up": 3, "near_down": 3, "join": 6, "line": 12, "last": 27},
)


def mm(a, b, ca, cb):
    return lax.dot_general(a, b, (((ca,), (cb,)), ((), ())), preferred_element_type=F32)


def route(expert, idx_t, gate_t):
    picked = idx_t == expert
    gate = jnp.sum(jnp.where(picked, gate_t, 0.0), axis=0, keepdims=True)
    count = jnp.sum(jnp.where(picked, 1.0, 0.0), axis=0, keepdims=True)
    return picked, gate, count > 0.5


def expert_in(w, x_t, mask):
    d = x_t.shape[0]
    ab = mm(jnp.concatenate([w[:d], w[d : 2 * d]], axis=1), x_t, 0, 0)
    ab = jnp.where(mask, ab, 0.0)
    f = w.shape[1]
    return ab[:f], ab[f:]


def down(w, d):
    return jnp.concatenate([w[2 * d : 2 * d + d // 2], w[2 * d + d // 2 :]], axis=1)


def expert_forward(w, x_t, mask):
    d = x_t.shape[0]
    a, b = expert_in(w, x_t, mask)
    s = jax.nn.sigmoid(a)
    silu = a * s
    h = (silu * b).astype(BF16)
    o = mm(down(w, d), h, 0, 0).astype(BF16)
    return a, b, s, silu, h, o


def expert_backward(w, x, dy_t, gate, a, b, s, silu, h, o):
    d = x.shape[1]
    dy = dy_t.astype(F32)
    dgate = jnp.sum(dy * o.astype(F32), axis=0, keepdims=True)
    q = (gate * dy).astype(BF16)
    dh = mm(down(w, d), q, 1, 0)
    dw2 = mm(h, q, 1, 1)
    da = (dh * b * s * (1.0 + a * (1.0 - s))).astype(BF16)
    db = (dh * silu).astype(BF16)
    dab = jnp.concatenate([da, db], axis=0)
    dw13_t = mm(dab, x, 1, 0)
    du = mm(jnp.concatenate([w[:d], w[d : 2 * d]], axis=1), dab, 1, 0).astype(BF16)
    return dgate, dw13_t, dw2, du


def near_order(g):
    return g + lax.div(g, 2) * (1 - 2 * lax.rem(g, 2))


def far_order(g):
    return 2 - g + lax.div(g, 2) * (3 - 2 * lax.rem(g, 2))


def step_kernel(side, x_ref, dy_ref, ia_ref, ib_ref, ga_ref, gb_ref, w1a, w3a, w2a, w1b, w3b, w2b,
                xo_ref, dxi_ref, ta_ref, tb_ref, dga_ref, dgb_ref,
                wb, dwo, dws, rb, ah, af, bh, bf, xt, xm, xmt, dyt, acc, dxs,
                load_sem, ag_send, ag_recv, ag_pair, d_send, d_recv, pa_send, ah_recv, af_recv, pb_send, bh_recv, bf_recv):
    me = lax.axis_index("ep")
    core, chip = lax.rem(me, 2), lax.div(me, 2)
    cx, cy = lax.rem(chip, side), lax.div(chip, side)
    p = cx * (1 - core) + cy * core
    r = cy * (1 - core) + cx * core
    tok, d = x_ref.shape
    f = w1a.shape[2]
    wrows, grows = wb.shape[2], dwo.shape[2]
    wh, gh = wrows // 2, grows // 2
    steps = side * side
    ring = dws.shape[0]

    def member(i, j, c):
        return ((j * (1 - c) + i * c) * side + i * (1 - c) + j * c) * 2 + c

    def at(di, dj):
        return member(lax.rem(p + di, side), lax.rem(r + dj, side), core)

    sib = me + 1 - 2 * core
    first = {1: at(1, 0), -1: at(side - 1, 0)}
    second = {1: at(0, 1), -1: at(0, side - 1)}

    def rdma(src, dst, send, recv, dev):
        return pltpu.make_async_remote_copy(src_ref=src, dst_ref=dst, send_sem=send, recv_sem=recv, device_id={"ep": dev}, device_id_type=MESH)

    loads = []
    for layer, (w1, w3, w2) in enumerate(((w1a, w3a, w2a), (w1b, w3b, w2b))):
        parts = (w1.at[0], w3.at[0], w2.at[0, :, pl.ds(0, d // 2)], w2.at[0, :, pl.ds(d // 2, d // 2)])
        row = 0
        for n, part in enumerate(parts):
            loads.append(pltpu.make_async_copy(part, wb.at[layer, me, pl.ds(row, part.shape[0])], load_sem.at[4 * layer + n]))
            row += part.shape[0]
    for copy in loads:
        copy.start()

    barrier = pltpu.get_barrier_semaphore()
    for dev in (sib, *first.values(), *second.values()):
        pl.semaphore_signal(barrier, inc=1, device_id={"ep": dev}, device_id_type=MESH)
    pl.semaphore_wait(barrier, 5)

    ag_slots = []

    def ag_copy(layer, e, half, dev, pair=False):
        view = wb.at[layer, e] if half is None else wb.at[layer, e, pl.ds(half * wh, wh)]
        recv = ag_pair.at[layer, e] if pair else ag_recv.at[layer, e, half or 0]
        copy = rdma(view, view, ag_send.at[len(ag_slots)], recv, dev)
        ag_slots.append(half)
        copy.start()

    def ag_wait(layer, e, half):
        view = wb.at[layer, e] if half is None else wb.at[layer, e, pl.ds(half * wh, wh)]
        rdma(view, view, ag_send.at[0], ag_recv.at[layer, e, half or 0], me).wait_recv()

    def spread(layer, di):
        for dev in second.values():
            ag_copy(layer, at(di, 0), None, dev)

    def arrive(layer, di, dj):
        e = at(di, dj)
        last = dj or di
        if last == 2:
            ag_wait(layer, e, 0)
            ag_wait(layer, e, 1)
        elif last:
            ag_wait(layer, e, None)
        line = second if dj else first
        if last == 3:
            ag_copy(layer, e, 0, line[1])
        if last == 1:
            ag_copy(layer, e, 1, line[-1])
        ag_copy(layer, e, None, sib, pair=True)

    def own_out(layer):
        for dev in first.values():
            ag_copy(layer, me, None, dev)

    def pair_wait(layer, e):
        view = wb.at[layer, e]
        rdma(view, view, ag_send.at[0], ag_pair.at[layer, e], me).wait_recv()

    for copy in loads[:4]:
        copy.wait()
    own_out(0)
    arrive(0, 0, 0)
    xt[...] = x_ref[...].T
    dyt[...] = dy_ref[...].T
    acc[...] = xt[...].astype(F32)
    dxs[...] = dyt[...].astype(F32)
    dga_ref[...] = jnp.zeros_like(dga_ref)
    dgb_ref[...] = jnp.zeros_like(dgb_ref)
    for copy in loads[4:]:
        copy.wait()

    moves = {"spread": spread, "arrive": arrive, "own_out": own_out}

    def moves_at(k, base, half):
        for step in range(steps):
            todo = PLAN.get(base + 2 * step + half)
            if todo:
                @pl.when(k == step)
                def _():
                    for name, *args in todo:
                        moves[name](*args)

    def pick(order, k):
        a, b = order(lax.div(k, side)), order(lax.rem(k, side))
        return at(a, b), member(lax.rem(r + a, side), lax.rem(p + b, side), 1 - core)

    def forward_one(e):
        _, gate, mask = route(e, ia_ref[...], ga_ref[...])
        o = expert_forward(wb[0, e], xt[...], mask)[5]
        acc[...] += gate * o.astype(F32)

    def forward_body(k, carry):
        own, other = pick(near_order, k)
        moves_at(k, 0, 0)
        forward_one(own)
        moves_at(k, 0, 1)
        pair_wait(0, other)
        forward_one(other)
        return carry

    lax.fori_loop(0, steps, forward_body, 0)
    xmt[...] = acc[...].astype(BF16)
    xm[...] = xmt[...].T
    acc[...] = xmt[...].astype(F32)

    def pair_send(layer, k):
        slot = lax.rem(k, ring)
        return rdma(dws.at[slot], rb.at[layer, k], d_send.at[slot], d_recv.at[layer, k], sib)

    def join(layer, k):
        pair_send(layer, k).wait_recv()
        dwo[layer, k] += rb[layer, k]

    lo, hi = pl.ds(0, gh), pl.ds(gh, gh)

    def far_copies(layer, g):
        return (rdma(dwo.at[layer, 4 * g, lo], ah.at[layer, g, 0], pa_send.at[layer, g, 0], ah_recv.at[layer, g, 0], second[1]),
                rdma(dwo.at[layer, 4 * g, hi], ah.at[layer, g, 1], pa_send.at[layer, g, 1], ah_recv.at[layer, g, 1], second[-1]))

    def near_copies(layer, g):
        up, down = dwo.at[layer, 4 * g + 1], dwo.at[layer, 4 * g + 2]
        up_in, down_in = af.at[layer, g, 0], af.at[layer, g, 1]
        return tuple(
            rdma(src.at[part], dst.at[part], pa_send.at[layer, g, 2 + n], af_recv.at[layer, g, n], dev)
            for n, (src, dst, part, dev) in enumerate((
                (up, up_in, hi, second[1]), (up, up_in, lo, second[1]),
                (down, down_in, lo, second[-1]), (down, down_in, hi, second[-1]))))

    def line_far(layer):
        return (rdma(dwo.at[layer, 3, lo], bh.at[layer, 0], pb_send.at[layer, 0], bh_recv.at[layer, 0], first[1]),
                rdma(dwo.at[layer, 3, hi], bh.at[layer, 1], pb_send.at[layer, 1], bh_recv.at[layer, 1], first[-1]))

    def line_near(layer):
        return (rdma(dwo.at[layer, 7], bf.at[layer, 0], pb_send.at[layer, 2], bf_recv.at[layer, 0], first[1]),
                rdma(dwo.at[layer, 11], bf.at[layer, 1], pb_send.at[layer, 3], bf_recv.at[layer, 1], first[-1]))

    def add_far(layer, g):
        for n, copy in enumerate(far_copies(layer, g)):
            copy.wait_recv()
            part = pl.ds(n * gh, gh)
            dwo[layer, 4 * g + 1 + n, part] += ah[layer, g, n]

    def add_near(layer, g):
        for copy in near_copies(layer, g):
            copy.wait_recv()
        dwo[layer, 4 * g + 3] += af[layer, g, 0] + af[layer, g, 1]

    def add_line(layer, n):
        line_far(layer)[n].wait_recv()
        part = pl.ds(n * gh, gh)
        dwo[layer, 7 + 4 * n, part] += bh[layer, n]

    def finish(layer, out):
        add_near(layer, 3)
        for copy in line_near(layer):
            copy.wait_recv()
        out[...] = dwo[layer, 15] + bf[layer, 0] + bf[layer, 1]

    def when(cond, fn):
        if isinstance(cond, bool):
            if cond:
                fn()
        else:
            pl.when(cond)(fn)

    def each_group(kk, off, groups, fn):
        if isinstance(kk, int):
            if kk >= off and (kk - off) % 4 == 0 and (kk - off) // 4 < groups:
                fn((kk - off) // 4)
        else:
            pl.when((kk >= off) & (lax.rem(kk - off + 32, 4) == 0) & (kk < off + 4 * groups))(lambda: fn(lax.div(kk - off, 4)))

    def later(kk, first_step, last_step):
        return isinstance(kk, int) or (first_step < steps if kk is sweep[0] else last_step >= steps)

    def middle(layer, kk):
        at_ = SUMS[layer]
        if later(kk, at_["join"], at_["join"] + 12):
            each_group(kk, at_["join"], 4, functools.partial(add_far, layer))
        if later(kk, at_["line"], at_["line"] + 8):
            each_group(kk, at_["line"], 3, functools.partial(add_near, layer))
            when(kk == at_["line"] + 4, lambda: add_line(layer, 0))
            when(kk == at_["line"] + 8, lambda: add_line(layer, 1))
        if later(kk, at_["last"], at_["last"]):
            when(kk == at_["last"], lambda: finish(layer, (ta_ref, tb_ref)[layer]))

    def end(layer, kk):
        at_ = SUMS[layer]

        def start(copies, picks):
            def go(*g):
                made = copies(layer, *g)
                for n in picks:
                    made[n].start()
            return go

        for key, copies, picks in (("far", far_copies, (0, 1)), ("near_up", near_copies, (0,)), ("near_down", near_copies, (2,)), ("join", near_copies, (1, 3))):
            if later(kk, at_[key], at_[key] + 12):
                each_group(kk, at_[key], 4, start(copies, picks))
        if later(kk, at_["line"], at_["line"] + 8):
            when(kk == at_["line"], start(line_far, (0, 1)))
            when(kk == at_["line"] + 4, start(line_near, (0,)))
            when(kk == at_["line"] + 8, start(line_near, (1,)))

    def backward_one(layer, e, dst):
        idx, gates, dg = ((ia_ref, ga_ref, dga_ref), (ib_ref, gb_ref, dgb_ref))[layer]
        feat, rows = ((xt, x_ref), (xmt, xm))[layer]
        picked, gate, mask = route(e, idx[...], gates[...])
        w = wb[layer, e]
        parts = expert_forward(w, feat[...], mask)
        if layer:
            acc[...] += gate * parts[5].astype(F32)
        dgate, dw13_t, dw2, du = expert_backward(w, rows[...], dyt[...], gate, *parts)
        dg[...] += jnp.where(picked, dgate, 0.0)
        dst[: 2 * f] = dw13_t
        dst[2 * f :] = dw2
        dxs[...] += du.astype(F32)

    sweep = [None]

    def backward_body(layer, k, carry):
        sweep[0] = k
        own, other = pick(far_order, k)
        if layer:
            moves_at(k, 2 * steps, 0)
            pair_wait(1, other)

            @pl.when(k >= ring)
            def _():
                pair_send(layer, k).wait_send()
        else:
            pair_send(layer, k).wait_send()
        backward_one(layer, other, dws.at[lax.rem(k, ring)])
        if not layer:
            pl.when(k == 0)(lambda: join(1, steps - 1))
            middle(1, k + steps)
        pl.when(k >= 1)(lambda: join(layer, k - 1))
        middle(layer, k)
        pair_send(layer, k).start()
        if layer:
            moves_at(k, 2 * steps, 1)
        backward_one(layer, own, dwo.at[layer, k])
        if not layer:
            end(1, k + steps)
        end(layer, k)
        return carry

    lax.fori_loop(0, steps, functools.partial(backward_body, 1), 0)
    dyt[...] = dxs[...].astype(BF16)
    dxs[...] = dyt[...].astype(F32)
    xo_ref[...] = acc[...].astype(BF16)
    lax.fori_loop(0, steps, functools.partial(backward_body, 0), 0)
    dxi_ref[...] = dxs[...].astype(BF16)
    join(0, steps - 1)
    for kk in range(steps, SUMS[0]["last"] + 1):
        middle(0, kk)
        end(0, kk)

    for n, half in enumerate(ag_slots):
        view = wb.at[0, 0] if half is None else wb.at[0, 0, pl.ds(0, wh)]
        rdma(view, view, ag_send.at[n], ag_recv.at[0, 0, 0], me).wait_send()
    for k in range(steps - ring, steps):
        pair_send(0, k).wait_send()
    for layer in range(2):
        for g in range(side):
            for copy in far_copies(layer, g) + near_copies(layer, g):
                copy.wait_send()
        for copy in line_far(layer) + line_near(layer):
            copy.wait_send()


def finish_kernel(xo, dxi, ta, tb, dga, dgb, xo_ref, dxi_ref, dw1a, dw3a, dw2a, dw1b, dw3b, dw2b, dga_ref, dgb_ref):
    xo_ref[...] = xo[...].T
    dxi_ref[...] = dxi[...].T
    for total, dw1, dw3, dw2 in ((ta, dw1a, dw3a, dw2a), (tb, dw1b, dw3b, dw2b)):
        f = dw2.shape[1]
        dw1[0] = total[:f].T
        dw3[0] = total[f : 2 * f].T
        dw2[0] = total[2 * f :]
    dga_ref[...] = dga[...]
    dgb_ref[...] = dgb[...]


def solution(mesh):
    tok_spec = P(("dp", "ep"))
    w_spec = P("ep")
    members = mesh.shape["ep"]
    side = math.isqrt(members // 2)
    chips = side * side

    def device_program(x_in, idx_a, idx_b, gate_a, gate_b, dy_out, w1_a, w3_a, w2_a, w1_b, w3_b, w2_b):
        (tok, d), top, f = x_in.shape, idx_a.shape[1], w1_a.shape[2]
        vmem, any_ = pl.BlockSpec(memory_space=pltpu.VMEM), pl.BlockSpec(memory_space=pl.ANY)
        shape = jax.ShapeDtypeStruct
        rows, dgs = shape((tok, d), BF16), shape((top, tok), F32)
        dws = (shape((1, d, f), F32), shape((1, d, f), F32), shape((1, f, d), F32))
        cols = shape((d, tok), BF16)
        wrows, grows = 2 * d + 2 * f, 3 * f
        outs = pl.pallas_call(
            functools.partial(step_kernel, side),
            out_shape=(cols, cols, shape((grows, d), F32), shape((grows, d), F32), dgs, dgs),
            in_specs=[vmem] * 6 + [any_] * 6,
            out_specs=(vmem,) * 6,
            scratch_shapes=[
                pltpu.VMEM((2, members, wrows, f), BF16),
                pltpu.VMEM((2, chips, grows, d), F32),
                pltpu.VMEM((4, grows, d), F32),
                pltpu.VMEM((2, chips, grows, d), F32),
                pltpu.VMEM((2, side, 2, grows // 2, d), F32),
                pltpu.VMEM((2, side, 2, grows, d), F32),
                pltpu.VMEM((2, 2, grows // 2, d), F32),
                pltpu.VMEM((2, 2, grows, d), F32),
                pltpu.VMEM((d, tok), BF16),
                pltpu.VMEM((tok, d), BF16),
                pltpu.VMEM((d, tok), BF16),
                pltpu.VMEM((d, tok), BF16),
                pltpu.VMEM((d, tok), F32),
                pltpu.VMEM((d, tok), F32),
                pltpu.SemaphoreType.DMA((8,)),
                pltpu.SemaphoreType.DMA((72,)),
                pltpu.SemaphoreType.DMA((2, members, 2)),
                pltpu.SemaphoreType.DMA((2, members)),
                pltpu.SemaphoreType.DMA((4,)),
                pltpu.SemaphoreType.DMA((2, chips)),
                pltpu.SemaphoreType.DMA((2, side, 6)),
                pltpu.SemaphoreType.DMA((2, side, 2)),
                pltpu.SemaphoreType.DMA((2, side, 4)),
                pltpu.SemaphoreType.DMA((2, 4)),
                pltpu.SemaphoreType.DMA((2, 2)),
                pltpu.SemaphoreType.DMA((2, 2)),
            ],
            compiler_params=pltpu.CompilerParams(collective_id=0, has_side_effects=True, vmem_limit_bytes=62 * 2**20),
        )(x_in, dy_out, idx_a.T, idx_b.T, gate_a.T, gate_b.T, w1_a, w3_a, w2_a, w1_b, w3_b, w2_b)
        outs = pl.pallas_call(
            finish_kernel,
            out_shape=(rows, rows) + dws + dws + (dgs, dgs),
            in_specs=[vmem] * 6,
            out_specs=(vmem,) * 10,
        )(*outs)
        return tuple(outs[:8]) + (outs[8].T, outs[9].T)

    return jax.shard_map(device_program, mesh=mesh, in_specs=(tok_spec,) * 6 + (w_spec,) * 6, out_specs=(tok_spec,) * 10, check_vma=False)
```

```python
import functools
import math

import jax
import jax.numpy as jnp
from jax import lax
from jax.experimental import pallas as pl
from jax.experimental.pallas import tpu as pltpu
from jax.sharding import PartitionSpec as P

F32 = jnp.float32
BF16 = jnp.bfloat16
MESH = pl.DeviceIdType.MESH

PLAN = {
    0: (100, 3, 30, 10, 1,),
    1: (210, 230,),
    2: (2, 110, 130,),
    4: (11, 13,),
    5: (20, 220, 120, 320,),
    6: (33, 31,),
    7: (12,),
    8: (23,),
    10: (21,),
    11: (123, 121, 32, 310, 330,),
    13: (22,),
    15: (122,),
    16: (111, 113,),
    17: (300,),
    18: (112, 133, 131,),
    20: (103, 101,),
    22: (132,),
    26: (102,),
}
SUMS = (
    {"far": 2, "near_up": 4, "near_down": 4, "join": 7, "line": 16, "last": 30},
    {"far": 2, "near_up": 4, "near_down": 4, "join": 7, "line": 13, "last": 29},
)


def mm(a, b, ca, cb):
    return lax.dot_general(a, b, (((ca,), (cb,)), ((), ())), preferred_element_type=F32)


def route(expert, idx_t, gate_t):
    picked = idx_t == expert
    gate = jnp.sum(jnp.where(picked, gate_t, 0.0), axis=0, keepdims=True)
    count = jnp.sum(jnp.where(picked, 1.0, 0.0), axis=0, keepdims=True)
    return picked, gate, count > 0.5


def up_rows(w, d):
    return jnp.concatenate([w[:d], w[d : 2 * d]], axis=1)


def down_rows(w, d):
    return jnp.concatenate([w[2 * d : 2 * d + d // 2], w[2 * d + d // 2 :]], axis=1)


def forward_pair(experts, idx_t, gate_t, x_t, acc, ab, hid):
    d, f = x_t.shape[0], hid.shape[1]
    gates = []
    for n, w in enumerate(experts):
        _, gate, mask = route(w[0], idx_t, gate_t)
        gates.append(gate)
        ab[n] = jnp.where(mask, mm(up_rows(w[1], d), x_t, 0, 0), 0.0)
    for n in range(2):
        for row in range(0, f, 16):
            u = ab[n, row : row + 16]
            hid[n, row : row + 16] = (u * jax.nn.sigmoid(u) * ab[n, f + row : f + row + 16]).astype(BF16)
    parts = [gates[n] * mm(down_rows(w[1], d), hid[n], 0, 0).astype(BF16).astype(F32) for n, w in enumerate(experts)]
    acc[...] += parts[0] + parts[1]


def backward_pair(experts, idx_t, gate_t, x_t, x, dy_t, acc, dxs, dg, ab, hid, dhs, dab, q):
    d, f = x_t.shape[0], hid.shape[1]
    gates, picks = [], []
    for n, (e, w, _) in enumerate(experts):
        picked, gate, mask = route(e, idx_t, gate_t)
        gates.append(gate)
        picks.append(picked)
        q[n] = (gate * dy_t[...].astype(F32)).astype(BF16)
        ab[n] = jnp.where(mask, mm(up_rows(w, d), x_t[...], 0, 0), 0.0)
        dhs[n] = mm(down_rows(w, d), q[n], 1, 0)
    for n in range(2):
        for row in range(0, f, 16):
            u, v = ab[n, row : row + 16], ab[n, f + row : f + row + 16]
            dh = dhs[n, row : row + 16]
            s = jax.nn.sigmoid(u)
            silu = u * s
            hid[n, row : row + 16] = (silu * v).astype(BF16)
            dab[n, row : row + 16] = (dh * v * s * (1.0 + u * (1.0 - s))).astype(BF16)
            dab[n, f + row : f + row + 16] = (dh * silu).astype(BF16)
    for n, (e, w, dst) in enumerate(experts):
        dst[: 2 * f] = mm(dab[n], x[...], 1, 0)
        dst[2 * f :] = mm(hid[n], q[n], 1, 1)
    outs = [mm(down_rows(w, d), hid[n], 0, 0).astype(BF16).astype(F32) for n, (e, w, _) in enumerate(experts)]
    if acc is not None:
        acc[...] += gates[0] * outs[0] + gates[1] * outs[1]
    dy = dy_t[...].astype(F32)
    for n in range(2):
        dg[...] += jnp.where(picks[n], jnp.sum(dy * outs[n], axis=0, keepdims=True), 0.0)
    dus = [mm(up_rows(w, d), dab[n], 1, 0).astype(BF16).astype(F32) for n, (e, w, _) in enumerate(experts)]
    dxs[...] += dus[0] + dus[1]


def near_order(g):
    return g + lax.div(g, 2) * (1 - 2 * lax.rem(g, 2))


def far_order(g):
    return 2 - g + lax.div(g, 2) * (3 - 2 * lax.rem(g, 2))


def step_kernel(side, x_ref, dy_ref, ia_ref, ib_ref, ga_ref, gb_ref, w1a, w3a, w2a, w1b, w3b, w2b,
                xo_ref, dxi_ref, ta_ref, tb_ref, dga_ref, dgb_ref,
                wb, dwo, dws, rb, ah, af, bh, bf, xt, xm, xmt, dyt, acc, dxs, ab, hid, dhs, dab, q,
                load_sem, ag_send, ag_recv, ag_pair, d_send, d_recv, pa_send, ah_recv, af_recv, pb_send, bh_recv, bf_recv):
    me = lax.axis_index("ep")
    core, chip = lax.rem(me, 2), lax.div(me, 2)
    cx, cy = lax.rem(chip, side), lax.div(chip, side)
    p = cx * (1 - core) + cy * core
    r = cy * (1 - core) + cx * core
    tok, d = x_ref.shape
    f = w1a.shape[2]
    wrows, grows = wb.shape[2], dwo.shape[2]
    wh, gh = wrows // 2, grows // 2
    steps = side * side
    ring = dws.shape[0]

    def member(i, j, c):
        return ((j * (1 - c) + i * c) * side + i * (1 - c) + j * c) * 2 + c

    def at(di, dj):
        return member(lax.rem(p + di, side), lax.rem(r + dj, side), core)

    sib = me + 1 - 2 * core
    first = {1: at(1, 0), -1: at(side - 1, 0)}
    second = {1: at(0, 1), -1: at(0, side - 1)}

    def rdma(src, dst, send, recv, dev):
        return pltpu.make_async_remote_copy(src_ref=src, dst_ref=dst, send_sem=send, recv_sem=recv, device_id={"ep": dev}, device_id_type=MESH)

    loads = []
    for layer, (w1, w3, w2) in enumerate(((w1a, w3a, w2a), (w1b, w3b, w2b))):
        parts = (w1.at[0], w3.at[0], w2.at[0, :, pl.ds(0, d // 2)], w2.at[0, :, pl.ds(d // 2, d // 2)])
        row = 0
        for n, part in enumerate(parts):
            loads.append(pltpu.make_async_copy(part, wb.at[layer, me, pl.ds(row, part.shape[0])], load_sem.at[4 * layer + n]))
            row += part.shape[0]
    for copy in loads:
        copy.start()

    barrier = pltpu.get_barrier_semaphore()
    for dev in (sib, *first.values(), *second.values()):
        pl.semaphore_signal(barrier, inc=1, device_id={"ep": dev}, device_id_type=MESH)
    pl.semaphore_wait(barrier, 5)

    ag_slots = []

    def ag_copy(layer, e, half, dev, pair=False):
        view = wb.at[layer, e] if half is None else wb.at[layer, e, pl.ds(half * wh, wh)]
        recv = ag_pair.at[layer, e] if pair else ag_recv.at[layer, e, half or 0]
        copy = rdma(view, view, ag_send.at[len(ag_slots)], recv, dev)
        ag_slots.append(half)
        copy.start()

    def ag_wait(layer, e, half):
        view = wb.at[layer, e] if half is None else wb.at[layer, e, pl.ds(half * wh, wh)]
        rdma(view, view, ag_send.at[0], ag_recv.at[layer, e, half or 0], me).wait_recv()

    def spread(layer, di):
        for dev in second.values():
            ag_copy(layer, at(di, 0), None, dev)

    def arrive(layer, di, dj):
        e = at(di, dj)
        last = dj or di
        if last == 2:
            ag_wait(layer, e, 0)
            ag_wait(layer, e, 1)
        elif last:
            ag_wait(layer, e, None)
        line = second if dj else first
        if last == 3:
            ag_copy(layer, e, 0, line[1])
        if last == 1:
            ag_copy(layer, e, 1, line[-1])
        ag_copy(layer, e, None, sib, pair=True)

    def own_out(layer):
        for dev in first.values():
            ag_copy(layer, me, None, dev)

    def pair_wait(layer, e):
        view = wb.at[layer, e]
        rdma(view, view, ag_send.at[0], ag_pair.at[layer, e], me).wait_recv()

    for copy in loads[:4]:
        copy.wait()
    own_out(0)
    arrive(0, 0, 0)
    spread(0, 0)
    xt[...] = x_ref[...].T
    dyt[...] = dy_ref[...].T
    acc[...] = xt[...].astype(F32)
    dxs[...] = dyt[...].astype(F32)
    dga_ref[...] = jnp.zeros_like(dga_ref)
    dgb_ref[...] = jnp.zeros_like(dgb_ref)
    for copy in loads[4:]:
        copy.wait()

    def moves_at(k, base):
        for step in range(steps):
            todo = PLAN.get(base + step)
            if todo:
                @pl.when(k == step)
                def _():
                    for code in todo:
                        kind, block = divmod(code, 100)
                        kind, layer = divmod(kind, 2)
                        di, dj = divmod(block, 10)
                        if kind == 1:
                            spread(layer, di)
                        else:
                            if not block:
                                own_out(layer)
                            arrive(layer, di, dj)

    def pick(order, k):
        a, b = order(lax.div(k, side)), order(lax.rem(k, side))
        return at(a, b), member(lax.rem(r + a, side), lax.rem(p + b, side), 1 - core)

    def forward_body(k, carry):
        moves_at(k, 0)
        own, other = pick(near_order, k)
        pair_wait(0, other)
        forward_pair([(e, wb[0, e]) for e in (own, other)], ia_ref[...], ga_ref[...], xt[...], acc, ab, hid)
        return carry

    lax.fori_loop(0, steps, forward_body, 0)
    xmt[...] = acc[...].astype(BF16)
    xm[...] = xmt[...].T
    acc[...] = xmt[...].astype(F32)

    def pair_send(layer, k):
        slot = lax.rem(k, ring)
        return rdma(dws.at[slot], rb.at[layer, k], d_send.at[slot], d_recv.at[layer, k], sib)

    def join(layer, k):
        pair_send(layer, k).wait_recv()
        dwo[layer, k] += rb[layer, k]

    lo, hi = pl.ds(0, gh), pl.ds(gh, gh)

    def far_copies(layer, g):
        return (rdma(dwo.at[layer, 4 * g, lo], ah.at[layer, g, 0], pa_send.at[layer, g, 0], ah_recv.at[layer, g, 0], second[1]),
                rdma(dwo.at[layer, 4 * g, hi], ah.at[layer, g, 1], pa_send.at[layer, g, 1], ah_recv.at[layer, g, 1], second[-1]))

    def near_copies(layer, g):
        up, down = dwo.at[layer, 4 * g + 1], dwo.at[layer, 4 * g + 2]
        up_in, down_in = af.at[layer, g, 0], af.at[layer, g, 1]
        return tuple(
            rdma(src.at[part], dst.at[part], pa_send.at[layer, g, 2 + n], af_recv.at[layer, g, n], dev)
            for n, (src, dst, part, dev) in enumerate((
                (up, up_in, hi, second[1]), (up, up_in, lo, second[1]),
                (down, down_in, lo, second[-1]), (down, down_in, hi, second[-1]))))

    def line_far(layer):
        return (rdma(dwo.at[layer, 3, lo], bh.at[layer, 0], pb_send.at[layer, 0], bh_recv.at[layer, 0], first[1]),
                rdma(dwo.at[layer, 3, hi], bh.at[layer, 1], pb_send.at[layer, 1], bh_recv.at[layer, 1], first[-1]))

    def line_near(layer):
        return (rdma(dwo.at[layer, 7], bf.at[layer, 0], pb_send.at[layer, 2], bf_recv.at[layer, 0], first[1]),
                rdma(dwo.at[layer, 11], bf.at[layer, 1], pb_send.at[layer, 3], bf_recv.at[layer, 1], first[-1]))

    def add_far(layer, g):
        for n, copy in enumerate(far_copies(layer, g)):
            copy.wait_recv()
            part = pl.ds(n * gh, gh)
            dwo[layer, 4 * g + 1 + n, part] += ah[layer, g, n]

    def add_near(layer, g):
        for copy in near_copies(layer, g):
            copy.wait_recv()
        dwo[layer, 4 * g + 3] += af[layer, g, 0] + af[layer, g, 1]

    def add_line(layer, n):
        line_far(layer)[n].wait_recv()
        part = pl.ds(n * gh, gh)
        dwo[layer, 7 + 4 * n, part] += bh[layer, n]

    def finish(layer, out):
        add_near(layer, 3)
        for copy in line_near(layer):
            copy.wait_recv()
        out[...] = dwo[layer, 15] + bf[layer, 0] + bf[layer, 1]

    def when(cond, fn):
        if isinstance(cond, bool):
            if cond:
                fn()
        else:
            pl.when(cond)(fn)

    def each_group(kk, off, groups, fn):
        if isinstance(kk, int):
            if kk >= off and (kk - off) % 4 == 0 and (kk - off) // 4 < groups:
                fn((kk - off) // 4)
        else:
            pl.when((kk >= off) & (lax.rem(kk - off + 32, 4) == 0) & (kk < off + 4 * groups))(lambda: fn(lax.div(kk - off, 4)))

    def later(kk, first_step, last_step):
        return isinstance(kk, int) or (first_step < steps if kk is sweep[0] else last_step >= steps)

    def middle(layer, kk):
        at_ = SUMS[layer]
        if later(kk, at_["join"], at_["join"] + 12):
            each_group(kk, at_["join"], 4, functools.partial(add_far, layer))
        if later(kk, at_["line"], at_["line"] + 8):
            each_group(kk, at_["line"], 3, functools.partial(add_near, layer))
            when(kk == at_["line"] + 4, lambda: add_line(layer, 0))
            when(kk == at_["line"] + 8, lambda: add_line(layer, 1))
        if later(kk, at_["last"], at_["last"]):
            when(kk == at_["last"], lambda: finish(layer, (ta_ref, tb_ref)[layer]))

    def end(layer, kk):
        at_ = SUMS[layer]

        def start(copies, picks):
            def go(*g):
                made = copies(layer, *g)
                for n in picks:
                    made[n].start()
            return go

        for key, copies, picks in (("far", far_copies, (0, 1)), ("near_up", near_copies, (0,)), ("near_down", near_copies, (2,)), ("join", near_copies, (1, 3))):
            if later(kk, at_[key], at_[key] + 12):
                each_group(kk, at_[key], 4, start(copies, picks))
        if later(kk, at_["line"], at_["line"] + 8):
            when(kk == at_["line"], start(line_far, (0, 1)))
            when(kk == at_["line"] + 4, start(line_near, (0,)))
            when(kk == at_["line"] + 8, start(line_near, (1,)))

    sweep = [None]

    def backward_body(layer, k, carry):
        sweep[0] = k
        own, other = pick(far_order, k)
        if layer:
            moves_at(k, steps)
            pair_wait(1, other)

            @pl.when(k >= ring)
            def _():
                pair_send(layer, k).wait_send()
        else:
            pair_send(layer, k).wait_send()
            pl.when(k < 2)(lambda: join(1, k + steps - 2))
            middle(1, k + steps)
        pl.when(k >= 2)(lambda: join(layer, k - 2))
        middle(layer, k)
        experts = [(other, wb[layer, other], dws.at[lax.rem(k, ring)]), (own, wb[layer, own], dwo.at[layer, k])]
        idx, gates, dg, feat, rows = ((ia_ref, ga_ref, dga_ref, xt, x_ref), (ib_ref, gb_ref, dgb_ref, xmt, xm))[layer]
        backward_pair(experts, idx[...], gates[...], feat, rows, dyt, acc if layer else None, dxs, dg, ab, hid, dhs, dab, q)
        if not layer:
            end(1, k + steps)
        end(layer, k)
        pair_send(layer, k).start()
        return carry

    lax.fori_loop(0, steps, functools.partial(backward_body, 1), 0)
    dyt[...] = dxs[...].astype(BF16)
    dxs[...] = dyt[...].astype(F32)
    xo_ref[...] = acc[...].astype(BF16)
    lax.fori_loop(0, steps, functools.partial(backward_body, 0), 0)
    dxi_ref[...] = dxs[...].astype(BF16)
    for kk in range(steps, SUMS[0]["last"] + 1):
        if kk < steps + 2:
            join(0, kk - 2)
        middle(0, kk)
        end(0, kk)

    for n, half in enumerate(ag_slots):
        view = wb.at[0, 0] if half is None else wb.at[0, 0, pl.ds(0, wh)]
        rdma(view, view, ag_send.at[n], ag_recv.at[0, 0, 0], me).wait_send()
    for k in range(steps - ring, steps):
        pair_send(0, k).wait_send()
    for layer in range(2):
        for g in range(side):
            for copy in far_copies(layer, g) + near_copies(layer, g):
                copy.wait_send()
        for copy in line_far(layer) + line_near(layer):
            copy.wait_send()


def finish_kernel(xo, dxi, ta, tb, dga, dgb, xo_ref, dxi_ref, dw1a, dw3a, dw2a, dw1b, dw3b, dw2b, dga_ref, dgb_ref):
    xo_ref[...] = xo[...].T
    dxi_ref[...] = dxi[...].T
    for total, dw1, dw3, dw2 in ((ta, dw1a, dw3a, dw2a), (tb, dw1b, dw3b, dw2b)):
        f = dw2.shape[1]
        dw1[0] = total[:f].T
        dw3[0] = total[f : 2 * f].T
        dw2[0] = total[2 * f :]
    dga_ref[...] = dga[...]
    dgb_ref[...] = dgb[...]


def solution(mesh):
    tok_spec = P(("dp", "ep"))
    w_spec = P("ep")
    members = mesh.shape["ep"]
    side = math.isqrt(members // 2)
    chips = side * side

    def device_program(x_in, idx_a, idx_b, gate_a, gate_b, dy_out, w1_a, w3_a, w2_a, w1_b, w3_b, w2_b):
        (tok, d), top, f = x_in.shape, idx_a.shape[1], w1_a.shape[2]
        vmem, any_ = pl.BlockSpec(memory_space=pltpu.VMEM), pl.BlockSpec(memory_space=pl.ANY)
        shape = jax.ShapeDtypeStruct
        rows, dgs = shape((tok, d), BF16), shape((top, tok), F32)
        dws = (shape((1, d, f), F32), shape((1, d, f), F32), shape((1, f, d), F32))
        cols = shape((d, tok), BF16)
        wrows, grows = 2 * d + 2 * f, 3 * f
        outs = pl.pallas_call(
            functools.partial(step_kernel, side),
            out_shape=(cols, cols, shape((grows, d), F32), shape((grows, d), F32), dgs, dgs),
            in_specs=[vmem] * 6 + [any_] * 6,
            out_specs=(vmem,) * 6,
            scratch_shapes=[
                pltpu.VMEM((2, members, wrows, f), BF16),
                pltpu.VMEM((2, chips, grows, d), F32),
                pltpu.VMEM((4, grows, d), F32),
                pltpu.VMEM((2, chips, grows, d), F32),
                pltpu.VMEM((2, side, 2, grows // 2, d), F32),
                pltpu.VMEM((2, side, 2, grows, d), F32),
                pltpu.VMEM((2, 2, grows // 2, d), F32),
                pltpu.VMEM((2, 2, grows, d), F32),
                pltpu.VMEM((d, tok), BF16),
                pltpu.VMEM((tok, d), BF16),
                pltpu.VMEM((d, tok), BF16),
                pltpu.VMEM((d, tok), BF16),
                pltpu.VMEM((d, tok), F32),
                pltpu.VMEM((d, tok), F32),
                pltpu.VMEM((2, 2 * f, tok), F32),
                pltpu.VMEM((2, f, tok), BF16),
                pltpu.VMEM((2, f, tok), F32),
                pltpu.VMEM((2, 2 * f, tok), BF16),
                pltpu.VMEM((2, d, tok), BF16),
                pltpu.SemaphoreType.DMA((8,)),
                pltpu.SemaphoreType.DMA((72,)),
                pltpu.SemaphoreType.DMA((2, members, 2)),
                pltpu.SemaphoreType.DMA((2, members)),
                pltpu.SemaphoreType.DMA((4,)),
                pltpu.SemaphoreType.DMA((2, chips)),
                pltpu.SemaphoreType.DMA((2, side, 6)),
                pltpu.SemaphoreType.DMA((2, side, 2)),
                pltpu.SemaphoreType.DMA((2, side, 4)),
                pltpu.SemaphoreType.DMA((2, 4)),
                pltpu.SemaphoreType.DMA((2, 2)),
                pltpu.SemaphoreType.DMA((2, 2)),
            ],
            compiler_params=pltpu.CompilerParams(collective_id=0, has_side_effects=True, vmem_limit_bytes=62 * 2**20),
        )(x_in, dy_out, idx_a.T, idx_b.T, gate_a.T, gate_b.T, w1_a, w3_a, w2_a, w1_b, w3_b, w2_b)
        outs = pl.pallas_call(
            finish_kernel,
            out_shape=(rows, rows) + dws + dws + (dgs, dgs),
            in_specs=[vmem] * 6,
            out_specs=(vmem,) * 10,
        )(*outs)
        return tuple(outs[:8]) + (outs[8].T, outs[9].T)

    return jax.shard_map(device_program, mesh=mesh, in_specs=(tok_spec,) * 6 + (w_spec,) * 6, out_specs=(tok_spec,) * 10, check_vma=False)
```

```python
import functools
import math

import jax
import jax.numpy as jnp
from jax import lax
from jax.experimental import pallas as pl
from jax.experimental.pallas import tpu as pltpu
from jax.sharding import PartitionSpec as P

F32 = jnp.float32
BF16 = jnp.bfloat16
MESH = pl.DeviceIdType.MESH

PLAN = {
    0: (100, 1, 30,),
    1: (3, 10,),
    2: (210, 230,),
    3: (2, 110, 20, 130,),
    4: (13,),
    5: (11, 220,),
    6: (33, 31,),
    7: (12, 120, 320,),
    8: (21, 23,),
    9: (310, 32,),
    12: (121, 123,),
    13: (22,),
    14: (330,),
    16: (122, 111, 113, 300,),
    17: (131, 133,),
    18: (112,),
    20: (101, 103,),
    21: (132,),
    26: (102,),
}
SUMS = (
    {"far": 2, "near_up": 7, "near_down": 7, "join": 8, "line": 22, "last": 31},
    {"far": 2, "near_up": 4, "near_down": 4, "join": 7, "line": 12, "last": 31},
)


def mm(a, b, ca, cb):
    return lax.dot_general(a, b, (((ca,), (cb,)), ((), ())), preferred_element_type=F32)


def route(expert, idx_t, gate_t):
    picked = idx_t == expert
    gate = jnp.sum(jnp.where(picked, gate_t, 0.0), axis=0, keepdims=True)
    count = jnp.sum(jnp.where(picked, 1.0, 0.0), axis=0, keepdims=True)
    return picked, gate, count > 0.5


def up_rows(w, d):
    return jnp.concatenate([w[pl.ds(0, d)], w[pl.ds(d, d)]], axis=1)


def down_rows(w, d):
    return jnp.concatenate([w[pl.ds(2 * d, d // 2)], w[pl.ds(2 * d + d // 2, d // 2)]], axis=1)


def strips(rows):
    return [pl.ds(row, 16) for row in range(0, rows, 16)]


def forward_pair(experts, idx_t, gate_t, x_t, acc, ab, hid, o16):
    d, f = x_t.shape[0], hid.shape[1]
    gates = []
    for n, (e, w) in enumerate(experts):
        _, gate, mask = route(e, idx_t, gate_t)
        gates.append(gate)
        ab[n] = jnp.where(mask, mm(up_rows(w, d), x_t[...], 0, 0), 0.0)
    for n, (e, w) in enumerate(experts):
        for row in range(0, f, 16):
            u = ab[n, row : row + 16]
            hid[n, row : row + 16] = (u * jax.nn.sigmoid(u) * ab[n, f + row : f + row + 16]).astype(BF16)
        o16[n] = mm(down_rows(w, d), hid[n], 0, 0).astype(BF16)
    for part in strips(d):
        acc[part] += gates[0] * o16[0, part].astype(F32) + gates[1] * o16[1, part].astype(F32)


def backward_pair(experts, idx_t, gate_t, x_t, x, dy_t, acc, dxs, dg, ab, hid, dhs, dab, q, o16, du16):
    d, f = x_t.shape[0], hid.shape[1]
    gates, picks = [], []
    for n, (e, w, _) in enumerate(experts):
        picked, gate, mask = route(e, idx_t, gate_t)
        gates.append(gate)
        picks.append(picked)
        for part in strips(d):
            q[n, part] = (gate * dy_t[part].astype(F32)).astype(BF16)
        ab[n] = jnp.where(mask, mm(up_rows(w, d), x_t[...], 0, 0), 0.0)
        dhs[n] = mm(down_rows(w, d), q[n], 1, 0)
    for n, (e, w, dst) in enumerate(experts):
        for row in range(0, f, 16):
            u, v = ab[n, row : row + 16], ab[n, f + row : f + row + 16]
            dh = dhs[n, row : row + 16]
            s = jax.nn.sigmoid(u)
            silu = u * s
            hid[n, row : row + 16] = (silu * v).astype(BF16)
            dab[n, row : row + 16] = (dh * v * s * (1.0 + u * (1.0 - s))).astype(BF16)
            dab[n, f + row : f + row + 16] = (dh * silu).astype(BF16)
        o16[n] = mm(down_rows(w, d), hid[n], 0, 0).astype(BF16)
        du16[n] = mm(up_rows(w, d), dab[n], 1, 0).astype(BF16)
        dst[: 2 * f] = mm(dab[n], x[...], 1, 0)
        dst[2 * f :] = mm(hid[n], q[n], 1, 1)
    sums = [0.0, 0.0]
    for part in strips(d):
        dy = dy_t[part].astype(F32)
        outs = [o16[n, part].astype(F32) for n in range(2)]
        if acc is not None:
            acc[part] += gates[0] * outs[0] + gates[1] * outs[1]
        for n in range(2):
            prod = dy * outs[n]
            sums[n] = sums[n] + (prod[:8] + prod[8:])
        dxs[part] += du16[0, part].astype(F32) + du16[1, part].astype(F32)
    dg[...] += jnp.where(picks[0], jnp.sum(sums[0], axis=0, keepdims=True), 0.0) + jnp.where(picks[1], jnp.sum(sums[1], axis=0, keepdims=True), 0.0)


def near_order(g):
    return g + lax.div(g, 2) * (1 - 2 * lax.rem(g, 2))


def far_order(g):
    return 2 - g + lax.div(g, 2) * (3 - 2 * lax.rem(g, 2))


def step_kernel(side, x_in, dy_in, ia_in, ib_in, ga_in, gb_in, w1a, w3a, w2a, w1b, w3b, w2b,
                xo_out, dxi_out, ta_out, tb_out, dga_out, dgb_out,
                x_ref, dy_ref, ia_ref, ib_ref, ga_ref, gb_ref, xo_ref, ta_ref, tb_ref, dga_ref, dgb_ref, in_sem, out_sem, wb, dwo, dws, rb, ah, af, bh, bf, xt, xm, xmt, dyt, acc, dxs, ab, hid, dhs, dab, q, o16, du16,
                load_sem, ag_send, ag_recv, ag_pair, d_send, d_recv, pa_send, ah_recv, af_recv, pb_send, bh_recv, bf_recv):
    me = lax.axis_index("ep")
    core, chip = lax.rem(me, 2), lax.div(me, 2)
    cx, cy = lax.rem(chip, side), lax.div(chip, side)
    p = cx * (1 - core) + cy * core
    r = cy * (1 - core) + cx * core
    tok, d = x_ref.shape
    f = w1a.shape[2]
    wrows, grows = wb.shape[2], dwo.shape[2]
    wh, gh = wrows // 2, grows // 2
    steps = side * side
    ring = dws.shape[0]

    def member(i, j, c):
        return ((j * (1 - c) + i * c) * side + i * (1 - c) + j * c) * 2 + c

    def at(di, dj):
        return member(lax.rem(p + di, side), lax.rem(r + dj, side), core)

    sib = me + 1 - 2 * core
    first = {1: at(1, 0), -1: at(side - 1, 0)}
    second = {1: at(0, 1), -1: at(0, side - 1)}

    def rdma(src, dst, send, recv, dev):
        return pltpu.make_async_remote_copy(src_ref=src, dst_ref=dst, send_sem=send, recv_sem=recv, device_id={"ep": dev}, device_id_type=MESH)

    loads = []
    for layer, (w1, w3, w2) in enumerate(((w1a, w3a, w2a), (w1b, w3b, w2b))):
        parts = (w1.at[0], w3.at[0], w2.at[0, :, pl.ds(0, d // 2)], w2.at[0, :, pl.ds(d // 2, d // 2)])
        row = 0
        for n, part in enumerate(parts):
            loads.append(pltpu.make_async_copy(part, wb.at[layer, me, pl.ds(row, part.shape[0])], load_sem.at[4 * layer + n]))
            row += part.shape[0]
    for copy in loads:
        copy.start()

    barrier = pltpu.get_barrier_semaphore()
    tokens = [pltpu.make_async_copy(src, dst, in_sem.at[n]) for n, (src, dst) in enumerate((
        (x_in, x_ref), (ia_in, ia_ref), (ga_in, ga_ref), (dy_in, dy_ref), (ib_in, ib_ref), (gb_in, gb_ref)))]

    def put(n, src, dst):
        return pltpu.make_async_copy(src, dst, out_sem.at[n])

    for dev in (sib, *first.values(), *second.values()):
        pl.semaphore_signal(barrier, inc=1, device_id={"ep": dev}, device_id_type=MESH)
    for copy in tokens:
        copy.start()
    pl.semaphore_wait(barrier, 5)

    ag_slots = []

    def ag_copy(layer, e, half, dev, pair=False):
        view = wb.at[layer, e] if half is None else wb.at[layer, e, pl.ds(half * wh, wh)]
        recv = ag_pair.at[layer, e] if pair else ag_recv.at[layer, e, half or 0]
        copy = rdma(view, view, ag_send.at[len(ag_slots)], recv, dev)
        ag_slots.append(half)
        copy.start()

    def ag_wait(layer, e, half):
        view = wb.at[layer, e] if half is None else wb.at[layer, e, pl.ds(half * wh, wh)]
        rdma(view, view, ag_send.at[0], ag_recv.at[layer, e, half or 0], me).wait_recv()

    def spread(layer, di):
        for dev in second.values():
            ag_copy(layer, at(di, 0), None, dev)

    def arrive(layer, di, dj):
        e = at(di, dj)
        last = dj or di
        if last == 2:
            ag_wait(layer, e, 0)
            ag_wait(layer, e, 1)
        elif last:
            ag_wait(layer, e, None)
        line = second if dj else first
        if last == 3:
            ag_copy(layer, e, 0, line[1])
        if last == 1:
            ag_copy(layer, e, 1, line[-1])
        ag_copy(layer, e, None, sib, pair=True)

    def own_out(layer):
        for dev in first.values():
            ag_copy(layer, me, None, dev)

    def pair_wait(layer, e):
        view = wb.at[layer, e]
        rdma(view, view, ag_send.at[0], ag_pair.at[layer, e], me).wait_recv()

    for copy in loads[:4]:
        copy.wait()
    own_out(0)
    arrive(0, 0, 0)
    spread(0, 0)
    for copy in tokens:
        copy.wait()
    xt[...] = x_ref[...].T
    dyt[...] = dy_ref[...].T
    acc[...] = xt[...].astype(F32)
    dxs[...] = dyt[...].astype(F32)
    dga_ref[...] = jnp.zeros_like(dga_ref)
    dgb_ref[...] = jnp.zeros_like(dgb_ref)
    for copy in loads[4:]:
        copy.wait()

    def moves_at(k, base):
        for step in range(steps):
            todo = PLAN.get(base + step)
            if todo:
                @pl.when(k == step)
                def _():
                    for code in todo:
                        kind, block = divmod(code, 100)
                        kind, layer = divmod(kind, 2)
                        di, dj = divmod(block, 10)
                        if kind == 1:
                            spread(layer, di)
                        else:
                            if not block:
                                own_out(layer)
                            arrive(layer, di, dj)

    def pick(order, k):
        a, b = order(lax.div(k, side)), order(lax.rem(k, side))
        return at(a, b), member(lax.rem(r + a, side), lax.rem(p + b, side), 1 - core)

    def forward_body(k, carry):
        moves_at(k, 0)
        own, other = pick(near_order, k)
        pair_wait(0, other)
        forward_pair([(e, wb.at[0, e]) for e in (own, other)], ia_ref[...], ga_ref[...], xt, acc, ab, hid, o16)
        return carry

    lax.fori_loop(0, steps, forward_body, 0)
    xmt[...] = acc[...].astype(BF16)
    xm[...] = xmt[...].T
    acc[...] = xmt[...].astype(F32)

    def pair_send(layer, k):
        slot = lax.rem(k, ring)
        return rdma(dws.at[slot], rb.at[layer, k], d_send.at[slot], d_recv.at[layer, k], sib)

    def join(layer, k):
        pair_send(layer, k).wait_recv()
        dwo[layer, k] += rb[layer, k]

    lo, hi = pl.ds(0, gh), pl.ds(gh, gh)

    def far_copies(layer, g):
        return (rdma(dwo.at[layer, 4 * g, lo], ah.at[layer, g, 0], pa_send.at[layer, g, 0], ah_recv.at[layer, g, 0], second[1]),
                rdma(dwo.at[layer, 4 * g, hi], ah.at[layer, g, 1], pa_send.at[layer, g, 1], ah_recv.at[layer, g, 1], second[-1]))

    def near_copies(layer, g):
        up, down = dwo.at[layer, 4 * g + 1], dwo.at[layer, 4 * g + 2]
        up_in, down_in = af.at[layer, g, 0], af.at[layer, g, 1]
        return tuple(
            rdma(src.at[part], dst.at[part], pa_send.at[layer, g, 2 + n], af_recv.at[layer, g, n], dev)
            for n, (src, dst, part, dev) in enumerate((
                (up, up_in, hi, second[1]), (up, up_in, lo, second[1]),
                (down, down_in, lo, second[-1]), (down, down_in, hi, second[-1]))))

    def line_far(layer):
        return (rdma(dwo.at[layer, 3, lo], bh.at[layer, 0], pb_send.at[layer, 0], bh_recv.at[layer, 0], first[1]),
                rdma(dwo.at[layer, 3, hi], bh.at[layer, 1], pb_send.at[layer, 1], bh_recv.at[layer, 1], first[-1]))

    def line_near(layer):
        return (rdma(dwo.at[layer, 7], bf.at[layer, 0], pb_send.at[layer, 2], bf_recv.at[layer, 0], first[1]),
                rdma(dwo.at[layer, 11], bf.at[layer, 1], pb_send.at[layer, 3], bf_recv.at[layer, 1], first[-1]))

    def add_far(layer, g):
        for n, copy in enumerate(far_copies(layer, g)):
            copy.wait_recv()
            part = pl.ds(n * gh, gh)
            dwo[layer, 4 * g + 1 + n, part] += ah[layer, g, n]

    def add_near(layer, g):
        for copy in near_copies(layer, g):
            copy.wait_recv()
        dwo[layer, 4 * g + 3] += af[layer, g, 0] + af[layer, g, 1]

    def add_line(layer, n):
        line_far(layer)[n].wait_recv()
        part = pl.ds(n * gh, gh)
        dwo[layer, 7 + 4 * n, part] += bh[layer, n]

    def finish(layer, out):
        add_near(layer, 3)
        for copy in line_near(layer):
            copy.wait_recv()
        out[...] = dwo[layer, 15] + bf[layer, 0] + bf[layer, 1]

    def when(cond, fn):
        if isinstance(cond, bool):
            if cond:
                fn()
        else:
            pl.when(cond)(fn)

    def each_group(kk, off, groups, fn):
        if isinstance(kk, int):
            if kk >= off and (kk - off) % 4 == 0 and (kk - off) // 4 < groups:
                fn((kk - off) // 4)
        else:
            pl.when((kk >= off) & (lax.rem(kk - off + 32, 4) == 0) & (kk < off + 4 * groups))(lambda: fn(lax.div(kk - off, 4)))

    def later(kk, first_step, last_step):
        return isinstance(kk, int) or (first_step < steps if kk is sweep[0] else last_step >= steps)

    def middle(layer, kk):
        at_ = SUMS[layer]
        if later(kk, at_["join"], at_["join"] + 12):
            each_group(kk, at_["join"], 4, functools.partial(add_far, layer))
        if later(kk, at_["line"], at_["line"] + 8):
            each_group(kk, at_["line"], 3, functools.partial(add_near, layer))
            when(kk == at_["line"] + 4, lambda: add_line(layer, 0))
            when(kk == at_["line"] + 8, lambda: add_line(layer, 1))
        if later(kk, at_["last"], at_["last"]):
            when(kk == at_["last"], lambda: finish(layer, (ta_ref, tb_ref)[layer]))

    def end(layer, kk):
        at_ = SUMS[layer]

        def start(copies, picks):
            def go(*g):
                made = copies(layer, *g)
                for n in picks:
                    made[n].start()
            return go

        for key, copies, picks in (("far", far_copies, (0, 1)), ("near_up", near_copies, (0,)), ("near_down", near_copies, (2,)), ("join", near_copies, (1, 3))):
            if later(kk, at_[key], at_[key] + 12):
                each_group(kk, at_[key], 4, start(copies, picks))
        if later(kk, at_["line"], at_["line"] + 8):
            when(kk == at_["line"], start(line_far, (0, 1)))
            when(kk == at_["line"] + 4, start(line_near, (0,)))
            when(kk == at_["line"] + 8, start(line_near, (1,)))

    sweep = [None]

    def backward_body(layer, k, carry):
        sweep[0] = k
        own, other = pick(far_order, k)
        if layer:
            moves_at(k, steps)
            pair_wait(1, other)

            @pl.when(k >= ring)
            def _():
                pair_send(layer, k).wait_send()
        else:
            pair_send(layer, k).wait_send()
            pl.when(k < 2)(lambda: join(1, k + steps - 2))
            middle(1, k + steps)
        pl.when(k >= 2)(lambda: join(layer, k - 2))
        middle(layer, k)
        experts = [(other, wb.at[layer, other], dws.at[lax.rem(k, ring)]), (own, wb.at[layer, own], dwo.at[layer, k])]
        idx, gates, dg, feat, rows = ((ia_ref, ga_ref, dga_ref, xt, x_ref), (ib_ref, gb_ref, dgb_ref, xmt, xm))[layer]
        backward_pair(experts, idx[...], gates[...], feat, rows, dyt, acc if layer else None, dxs, dg, ab, hid, dhs, dab, q, o16, du16)
        if not layer:
            end(1, k + steps)
        end(layer, k)
        pair_send(layer, k).start()
        return carry

    lax.fori_loop(0, steps, functools.partial(backward_body, 1), 0)
    dyt[...] = dxs[...].astype(BF16)
    dxs[...] = dyt[...].astype(F32)
    xo_ref[...] = acc[...].astype(BF16)
    lax.fori_loop(0, steps, functools.partial(backward_body, 0), 0)
    results = [put(0, xo_ref, xo_out), put(1, tb_ref, tb_out), put(2, dgb_ref, dgb_out)]
    dyt[...] = dxs[...].astype(BF16)
    results += [put(3, dyt, dxi_out), put(4, dga_ref, dga_out)]
    for kk in range(steps, SUMS[0]["last"] + 1):
        if kk < steps + 2:
            join(0, kk - 2)
        middle(0, kk)
        end(0, kk)
        if kk == steps + 1:
            for copy in results:
                copy.start()

    results.append(put(5, ta_ref, ta_out))
    results[-1].start()
    for n, half in enumerate(ag_slots):
        view = wb.at[0, 0] if half is None else wb.at[0, 0, pl.ds(0, wh)]
        rdma(view, view, ag_send.at[n], ag_recv.at[0, 0, 0], me).wait_send()
    for k in range(steps - ring, steps):
        pair_send(0, k).wait_send()
    for layer in range(2):
        for g in range(side):
            for copy in far_copies(layer, g) + near_copies(layer, g):
                copy.wait_send()
        for copy in line_far(layer) + line_near(layer):
            copy.wait_send()
    for copy in results:
        copy.wait()


def finish_kernel(xo_in, dxi_in, ta_in, tb_in, dga_in, dgb_in, xo_ref, dxi_ref, dw1a, dw3a, dw2a, dw1b, dw3b, dw2b, dga_ref, dgb_ref,
                  xo, dxi, ta, tb, dga, dgb, rows, dws, in_sem, out_sem):
    pairs = ((tb_in, tb), (xo_in, xo), (ta_in, ta), (dxi_in, dxi), (dga_in, dga), (dgb_in, dgb))
    loads = [pltpu.make_async_copy(src, dst, in_sem.at[n]) for n, (src, dst) in enumerate(pairs)]
    for copy in loads:
        copy.start()
    stores = []

    def put(src, dst):
        stores.append(pltpu.make_async_copy(src, dst, out_sem.at[len(stores)]))
        stores[-1].start()

    f = dw2a.shape[1]
    work = ((tb, dw1b, dw3b, dw2b, xo, xo_ref), (ta, dw1a, dw3a, dw2a, dxi, dxi_ref))
    for n, (total, dw1, dw3, dw2, cols, out) in enumerate(work):
        loads[2 * n].wait()
        put(total.at[pl.ds(2 * f, f)], dw2.at[0])
        for m, dw in enumerate((dw1, dw3)):
            dws[2 * n + m] = total[m * f : (m + 1) * f].T
        loads[2 * n + 1].wait()
        rows[n] = cols[...].T
        for m, dw in enumerate((dw1, dw3)):
            put(dws.at[2 * n + m], dw.at[0])
        loads[4 + n].wait()
        put((dga, dgb)[n], (dga_ref, dgb_ref)[n])
        put(rows.at[n], out)
    for copy in stores:
        copy.wait()


def solution(mesh):
    tok_spec = P(("dp", "ep"))
    w_spec = P("ep")
    members = mesh.shape["ep"]
    side = math.isqrt(members // 2)
    chips = side * side

    def device_program(x_in, idx_a, idx_b, gate_a, gate_b, dy_out, w1_a, w3_a, w2_a, w1_b, w3_b, w2_b):
        (tok, d), top, f = x_in.shape, idx_a.shape[1], w1_a.shape[2]
        any_ = pl.BlockSpec(memory_space=pl.ANY)
        shape = jax.ShapeDtypeStruct
        rows, dgs = shape((tok, d), BF16), shape((top, tok), F32)
        dws = (shape((1, d, f), F32), shape((1, d, f), F32), shape((1, f, d), F32))
        cols = shape((d, tok), BF16)
        wrows, grows = 2 * d + 2 * f, 3 * f
        outs = pl.pallas_call(
            functools.partial(step_kernel, side),
            out_shape=(cols, cols, shape((grows, d), F32), shape((grows, d), F32), dgs, dgs),
            in_specs=[any_] * 12,
            out_specs=(any_,) * 6,
            scratch_shapes=[
                pltpu.VMEM((tok, d), BF16),
                pltpu.VMEM((tok, d), BF16),
                pltpu.VMEM((top, tok), jnp.int32),
                pltpu.VMEM((top, tok), jnp.int32),
                pltpu.VMEM((top, tok), F32),
                pltpu.VMEM((top, tok), F32),
                pltpu.VMEM((d, tok), BF16),
                pltpu.VMEM((grows, d), F32),
                pltpu.VMEM((grows, d), F32),
                pltpu.VMEM((top, tok), F32),
                pltpu.VMEM((top, tok), F32),
                pltpu.SemaphoreType.DMA((6,)),
                pltpu.SemaphoreType.DMA((6,)),
                pltpu.VMEM((2, members, wrows, f), BF16),
                pltpu.VMEM((2, chips, grows, d), F32),
                pltpu.VMEM((4, grows, d), F32),
                pltpu.VMEM((2, chips, grows, d), F32),
                pltpu.VMEM((2, side, 2, grows // 2, d), F32),
                pltpu.VMEM((2, side, 2, grows, d), F32),
                pltpu.VMEM((2, 2, grows // 2, d), F32),
                pltpu.VMEM((2, 2, grows, d), F32),
                pltpu.VMEM((d, tok), BF16),
                pltpu.VMEM((tok, d), BF16),
                pltpu.VMEM((d, tok), BF16),
                pltpu.VMEM((d, tok), BF16),
                pltpu.VMEM((d, tok), F32),
                pltpu.VMEM((d, tok), F32),
                pltpu.VMEM((2, 2 * f, tok), F32),
                pltpu.VMEM((2, f, tok), BF16),
                pltpu.VMEM((2, f, tok), F32),
                pltpu.VMEM((2, 2 * f, tok), BF16),
                pltpu.VMEM((2, d, tok), BF16),
                pltpu.VMEM((2, d, tok), BF16),
                pltpu.VMEM((2, d, tok), BF16),
                pltpu.SemaphoreType.DMA((8,)),
                pltpu.SemaphoreType.DMA((72,)),
                pltpu.SemaphoreType.DMA((2, members, 2)),
                pltpu.SemaphoreType.DMA((2, members)),
                pltpu.SemaphoreType.DMA((4,)),
                pltpu.SemaphoreType.DMA((2, chips)),
                pltpu.SemaphoreType.DMA((2, side, 6)),
                pltpu.SemaphoreType.DMA((2, side, 2)),
                pltpu.SemaphoreType.DMA((2, side, 4)),
                pltpu.SemaphoreType.DMA((2, 4)),
                pltpu.SemaphoreType.DMA((2, 2)),
                pltpu.SemaphoreType.DMA((2, 2)),
            ],
            compiler_params=pltpu.CompilerParams(collective_id=0, has_side_effects=True, vmem_limit_bytes=62 * 2**20),
        )(x_in, dy_out, idx_a.T, idx_b.T, gate_a.T, gate_b.T, w1_a, w3_a, w2_a, w1_b, w3_b, w2_b)
        outs = pl.pallas_call(
            finish_kernel,
            out_shape=(rows, rows) + dws + dws + (dgs, dgs),
            in_specs=[any_] * 6,
            out_specs=(any_,) * 10,
            scratch_shapes=[
                pltpu.VMEM((d, tok), BF16),
                pltpu.VMEM((d, tok), BF16),
                pltpu.VMEM((grows, d), F32),
                pltpu.VMEM((grows, d), F32),
                pltpu.VMEM((top, tok), F32),
                pltpu.VMEM((top, tok), F32),
                pltpu.VMEM((2, tok, d), BF16),
                pltpu.VMEM((4, d, f), F32),
                pltpu.SemaphoreType.DMA((6,)),
                pltpu.SemaphoreType.DMA((10,)),
            ],
        )(*outs)
        return tuple(outs[:8]) + (outs[8].T, outs[9].T)

    return jax.shard_map(device_program, mesh=mesh, in_specs=(tok_spec,) * 6 + (w_spec,) * 6, out_specs=(tok_spec,) * 10, check_vma=False)
```

```python
import functools
import math

import jax
import jax.numpy as jnp
from jax import lax
from jax.experimental import pallas as pl
from jax.experimental.pallas import tpu as pltpu
from jax.sharding import PartitionSpec as P

F32 = jnp.float32
BF16 = jnp.bfloat16
MESH = pl.DeviceIdType.MESH

PLAN = {
    0: (100, 10, 210, 30, 1,),
    1: (3,),
    2: (230, 20, 13, 11,),
    3: (220, 2,),
    4: (31,),
    5: (33, 12,),
    6: (300,),
    8: (21, 23,),
    9: (32,),
    11: (110, 130,),
    12: (310,),
    13: (103, 22, 101,),
    15: (330,),
    17: (113, 111, 120,),
    18: (320, 102,),
    21: (112, 133, 131,),
    24: (121, 123,),
    25: (132,),
    29: (122,),
}
TOKENS = (
    {0: ((3,), (), ()), 5: ((), (1, 4, 5), ()), 11: ((), (3,), ()), 12: ((2,), (), ()), 15: ((), (), (1, 4, 5))},
    {13: ((1, 4, 5), (), ())},
    {1: ((), (), (0,))},
    {1: ((0,), (), (3,)), 4: ((), (2,), ()), 6: ((), (0,), ()), 7: ((), (), (2,))},
)


def mm(a, b, ca, cb):
    return lax.dot_general(a, b, (((ca,), (cb,)), ((), ())), preferred_element_type=F32)


def route(expert, idx_t, gate_t):
    picked = idx_t == expert
    gate = jnp.sum(jnp.where(picked, gate_t, 0.0), axis=0, keepdims=True)
    count = jnp.sum(jnp.where(picked, 1.0, 0.0), axis=0, keepdims=True)
    return picked, gate, count > 0.5


def up_rows(w, d):
    return jnp.concatenate([w[pl.ds(0, d)], w[pl.ds(d, d)]], axis=1)


def down_rows(w, d):
    return jnp.concatenate([w[pl.ds(2 * d, d // 2)], w[pl.ds(2 * d + d // 2, d // 2)]], axis=1)


def strips(rows):
    return [pl.ds(row, 16) for row in range(0, rows, 16)]


def forward_pair(experts, idx_t, gate_t, x_t, acc, ab, hid, o16):
    d, f = x_t.shape[0], hid.shape[1]
    gates = []
    for n, (e, w) in enumerate(experts):
        _, gate, mask = route(e, idx_t, gate_t)
        gates.append(gate)
        ab[n] = jnp.where(mask, mm(up_rows(w, d), x_t[...], 0, 0), 0.0)
    for n, (e, w) in enumerate(experts):
        for row in range(0, f, 16):
            u = ab[n, row : row + 16]
            hid[n, row : row + 16] = (u * jax.nn.sigmoid(u) * ab[n, f + row : f + row + 16]).astype(BF16)
        o16[n] = mm(down_rows(w, d), hid[n], 0, 0).astype(BF16)
    for part in strips(d):
        acc[part] += gates[0] * o16[0, part].astype(F32) + gates[1] * o16[1, part].astype(F32)


def hidden_grads(n, w, route_of, feat, dy_t, ab, hid, dhs, dab, q):
    d, f = feat.shape[0], hid.shape[1]
    _, gate, mask = route_of
    for part in strips(d):
        q[n, part] = (gate * dy_t[part].astype(F32)).astype(BF16)
    ab[n] = jnp.where(mask, mm(up_rows(w, d), feat[...], 0, 0), 0.0)
    dhs[n] = mm(down_rows(w, d), q[n], 1, 0)
    for row in range(0, f, 16):
        u, v = ab[n, row : row + 16], ab[n, f + row : f + row + 16]
        dh = dhs[n, row : row + 16]
        s = jax.nn.sigmoid(u)
        silu = u * s
        hid[n, row : row + 16] = (silu * v).astype(BF16)
        dab[n, row : row + 16] = (dh * v * (s + silu * (1.0 - s))).astype(BF16)
        dab[n, f + row : f + row + 16] = (dh * silu).astype(BF16)
    return gate


def token_pair(experts, idx_t, gate_t, feat, dy_t, acc, dxs, dg, ab, hid, dhs, dab, q, o16, du16):
    d = feat.shape[0]
    routes = [route(e, idx_t, gate_t) for e, _ in experts]
    gates = [hidden_grads(n, w, routes[n], feat, dy_t, ab, hid, dhs, dab, q) for n, (e, w) in enumerate(experts)]
    for n, (e, w) in enumerate(experts):
        o16[n] = mm(down_rows(w, d), hid[n], 0, 0).astype(BF16)
        du16[n] = mm(up_rows(w, d), dab[n], 1, 0).astype(BF16)
    sums = [0.0, 0.0]
    for part in strips(d):
        dy = dy_t[part].astype(F32)
        outs = [o16[n, part].astype(F32) for n in range(2)]
        if acc is not None:
            acc[part] += gates[0] * outs[0] + gates[1] * outs[1]
        for n in range(2):
            prod = dy * outs[n]
            sums[n] = sums[n] + (prod[:8] + prod[8:])
        dxs[part] += du16[0, part].astype(F32) + du16[1, part].astype(F32)
    terms = [jnp.where(routes[n][0], jnp.sum(sums[n], axis=0, keepdims=True), 0.0) for n in range(2)]
    dg[...] += terms[0] + terms[1]


def weight_part(e, w, sources, dst, ab, hid, dhs, dab, q):
    f = hid.shape[1]
    for n, (idx_t, gate_t, feat, x, dy_t) in enumerate(sources):
        hidden_grads(n, w, route(e, idx_t[...], gate_t[...]), feat, dy_t, ab, hid, dhs, dab, q)
    dst[: 2 * f] += sum(mm(dab[n], source[3][...], 1, 0) for n, source in enumerate(sources))
    dst[2 * f :] += sum(mm(hid[n], q[n], 1, 1) for n in range(len(sources)))


def near_order(g):
    return g + lax.div(g, 2) * (1 - 2 * lax.rem(g, 2))


def far_order(g):
    return 2 - g + lax.div(g, 2) * (3 - 2 * lax.rem(g, 2))


def step_kernel(side, x_in, dy_in, ia_in, ib_in, ga_in, gb_in, w1a, w3a, w2a, w1b, w3b, w2b,
                xo_out, dxi_out, ta_out, tb_out, dga_out, dgb_out,
                x_ref, xo_ref, ta_ref, tb_ref, dga_ref, dgb_ref, wb, tg, ri, rg, xn, dwo, bh, bf, acc, dxs, ab, hid, dhs, dab, q, o16, du16,
                in_sem, out_sem, load_sem, ag_send, ag_recv, ag_pair, tk_send, tk_recv, tk_pair, rs_send, bh_recv, bf_recv):
    me = lax.axis_index("ep")
    core, chip = lax.rem(me, 2), lax.div(me, 2)
    cx, cy = lax.rem(chip, side), lax.div(chip, side)
    p = cx * (1 - core) + cy * core
    r = cy * (1 - core) + cx * core
    tok, d = x_in.shape
    f = w1a.shape[2]
    wrows, grows = wb.shape[2], dwo.shape[2]
    wh, gh = wrows // 2, grows // 2
    steps = side * side

    def member(i, j, c):
        return ((j * (1 - c) + i * c) * side + i * (1 - c) + j * c) * 2 + c

    def at(di, dj):
        return member(lax.rem(p + di, side), lax.rem(r + dj, side), core)

    def near(dx, dy):
        return (lax.rem(cy + dy, side) * side + lax.rem(cx + dx, side)) * 2 + core

    def slot(dx):
        return lax.rem(cx + dx, side) * 2 + core

    sib = me + 1 - 2 * core
    xdev = {1: near(1, 0), -1: near(side - 1, 0)}
    ydev = {1: near(0, 1), -1: near(0, side - 1)}
    mine = slot(0)
    first = {1: at(1, 0), -1: at(side - 1, 0)}
    second = {1: at(0, 1), -1: at(0, side - 1)}

    def rdma(src, dst, send, recv, dev):
        return pltpu.make_async_remote_copy(src_ref=src, dst_ref=dst, send_sem=send, recv_sem=recv, device_id={"ep": dev}, device_id_type=MESH)

    loads = []
    for layer, (w1, w3, w2) in enumerate(((w1a, w3a, w2a), (w1b, w3b, w2b))):
        parts = (w1.at[0], w3.at[0], w2.at[0, :, pl.ds(0, d // 2)], w2.at[0, :, pl.ds(d // 2, d // 2)])
        row = 0
        for n, part in enumerate(parts):
            loads.append(pltpu.make_async_copy(part, wb.at[layer, me, pl.ds(row, part.shape[0])], load_sem.at[4 * layer + n]))
            row += part.shape[0]
    for copy in loads:
        copy.start()

    barrier = pltpu.get_barrier_semaphore()
    tokens = [pltpu.make_async_copy(src, dst, in_sem.at[n]) for n, (src, dst) in enumerate((
        (x_in, x_ref.at[0]), (dy_in, x_ref.at[1]), (ia_in, ri.at[mine, 0]), (ib_in, ri.at[mine, 1]), (ga_in, rg.at[mine, 0]), (gb_in, rg.at[mine, 1])))]

    def put(n, src, dst):
        return pltpu.make_async_copy(src, dst, out_sem.at[n])

    for dev in (sib, *first.values(), *second.values()):
        pl.semaphore_signal(barrier, inc=1, device_id={"ep": dev}, device_id_type=MESH)
    for copy in tokens:
        copy.start()
    pl.semaphore_wait(barrier, 5)

    ag_slots = []

    def ag_copy(layer, e, half, dev, pair=False):
        view = wb.at[layer, e] if half is None else wb.at[layer, e, pl.ds(half * wh, wh)]
        recv = ag_pair.at[layer, e] if pair else ag_recv.at[layer, e, half or 0]
        copy = rdma(view, view, ag_send.at[len(ag_slots)], recv, dev)
        ag_slots.append(half)
        copy.start()

    def ag_wait(layer, e, half):
        view = wb.at[layer, e] if half is None else wb.at[layer, e, pl.ds(half * wh, wh)]
        rdma(view, view, ag_send.at[0], ag_recv.at[layer, e, half or 0], me).wait_recv()

    def spread(layer, di):
        for dev in second.values():
            ag_copy(layer, at(di, 0), None, dev)

    def arrive(layer, di, dj):
        e = at(di, dj)
        last = dj or di
        if last == 2:
            ag_wait(layer, e, 0)
            ag_wait(layer, e, 1)
        elif last:
            ag_wait(layer, e, None)
        line = second if dj else first
        if last == 3:
            ag_copy(layer, e, 0, line[1])
        if last == 1:
            ag_copy(layer, e, 1, line[-1])
        ag_copy(layer, e, None, sib, pair=True)

    def own_out(layer):
        for dev in first.values():
            ag_copy(layer, me, None, dev)

    def pair_wait(layer, e):
        view = wb.at[layer, e]
        rdma(view, view, ag_send.at[0], ag_pair.at[layer, e], me).wait_recv()

    for copy in loads[:4]:
        copy.wait()
    own_out(0)
    arrive(0, 0, 0)
    spread(0, 0)
    for copy in tokens:
        copy.wait()
    tg[0, mine] = x_ref[0].T
    tg[3, mine] = x_ref[1].T
    acc[...] = tg[0, mine].astype(F32)
    dxs[...] = tg[3, mine].astype(F32)
    dga_ref[...] = jnp.zeros_like(dga_ref)
    dgb_ref[...] = jnp.zeros_like(dgb_ref)
    dwo[...] = jnp.zeros_like(dwo)
    for copy in loads[4:]:
        copy.wait()

    def block(a, s, half):
        ref = tg.at[a, s] if a < 4 else (ri, rg)[a - 4].at[s]
        rows = ref.shape[0] // 2
        return ref if half is None else ref.at[pl.ds(half * rows, rows)]

    def tk(a, s, half, n, dev, pair=False):
        view = block(a, s, half)
        return rdma(view, view, tk_send.at[a, n], tk_pair.at[a, s] if pair else tk_recv.at[a, s, half or 0], dev)

    def tk_out(a):
        return [tk(a, mine, None, 0, xdev[1]), tk(a, mine, None, 1, xdev[-1]), tk(a, mine, None, 2, sib, True)]

    def tk_next(a):
        return [tk(a, slot(3), 0, 3, xdev[1]), tk(a, slot(1), 1, 4, xdev[-1]), tk(a, slot(3), None, 5, sib, True), tk(a, slot(1), None, 6, sib, True)]

    def tk_last(a):
        return [tk(a, slot(2), None, 7, sib, True)]

    def tokens_at(k, table):
        for step, (out, step_on, last) in table.items():
            @pl.when(k == step)
            def _():
                for a in out:
                    for copy in tk_out(a):
                        copy.start()
                for a in step_on:
                    for s in (slot(3), slot(1)):
                        tk(a, s, None, 0, me).wait_recv()
                    for copy in tk_next(a):
                        copy.start()
                for a in last:
                    for half in range(2):
                        tk(a, slot(2), half, 0, me).wait_recv()
                    tk_last(a)[0].start()

    def moves_at(k, base):
        for step in range(steps):
            todo = PLAN.get(base + step)
            if todo:
                @pl.when(k == step)
                def _():
                    for code in todo:
                        kind, block = divmod(code, 100)
                        kind, layer = divmod(kind, 2)
                        di, dj = divmod(block, 10)
                        if kind == 1:
                            spread(layer, di)
                        else:
                            if not block:
                                own_out(layer)
                            arrive(layer, di, dj)

    def pick(order, k):
        a, b = order(lax.div(k, side)), order(lax.rem(k, side))
        return at(a, b), member(lax.rem(r + a, side), lax.rem(p + b, side), 1 - core)

    def forward_body(k, carry):
        moves_at(k, 0)
        own, other = pick(near_order, k)
        pair_wait(0, other)
        forward_pair([(e, wb.at[0, e]) for e in (own, other)], ri[mine, 0], rg[mine, 0], tg.at[0, mine], acc, ab, hid, o16)
        return carry

    lax.fori_loop(0, steps, forward_body, 0)
    tg[1, mine] = acc[...].astype(BF16)
    acc[...] = tg[1, mine].astype(F32)

    def token_body(layer, k, carry):
        own, other = pick(near_order, k)
        if layer:
            moves_at(k, steps)
            pair_wait(1, other)
        tokens_at(k, TOKENS[layer])
        experts = [(e, wb.at[layer, e]) for e in (own, other)]
        dg = (dga_ref, dgb_ref)[layer]
        token_pair(experts, ri[mine, layer], rg[mine, layer], tg.at[layer, mine], tg.at[2 + layer, mine], acc if layer else None, dxs, dg, ab, hid, dhs, dab, q, o16, du16)
        return carry

    lax.fori_loop(0, steps, functools.partial(token_body, 1), 0)
    tg[2, mine] = dxs[...].astype(BF16)
    dxs[...] = tg[2, mine].astype(F32)
    xo_ref[0] = acc[...].astype(BF16)
    lax.fori_loop(0, steps, functools.partial(token_body, 0), 0)
    xo_ref[1] = dxs[...].astype(BF16)

    lo, hi = pl.ds(0, gh), pl.ds(gh, gh)

    def sums(layer):
        up, down, far = dwo.at[layer, 1], dwo.at[layer, 2], dwo.at[layer, 0]
        parts = ((far.at[lo], bh.at[layer, 0], bh_recv.at[layer, 0], 1), (far.at[hi], bh.at[layer, 1], bh_recv.at[layer, 1], -1),
                 (up.at[hi], bf.at[layer, 0, hi], bf_recv.at[layer, 0], 1), (down.at[lo], bf.at[layer, 1, lo], bf_recv.at[layer, 1], -1),
                 (up.at[lo], bf.at[layer, 0, lo], bf_recv.at[layer, 2], 1), (down.at[hi], bf.at[layer, 1, hi], bf_recv.at[layer, 3], -1))
        return [rdma(src, dst, rs_send.at[layer, n], recv, ydev[way]) for n, (src, dst, recv, way) in enumerate(parts)]

    def add_far(layer):
        for n, copy in enumerate(sums(layer)[:2]):
            copy.wait_recv()
            part = pl.ds(n * gh, gh)
            dwo[layer, 1 + n, part] += bh[layer, n]

    def finish(layer, out):
        for copy in sums(layer)[2:]:
            copy.wait_recv()
        out[...] = dwo[layer, 3] + bf[layer, 0] + bf[layer, 1]

    def weight_body(layer, k, carry):
        n, half = lax.div(k, 2), lax.rem(k, 2)
        e = near(0, far_order(n))
        chips = [lax.rem(cx + near_order(2 * half + m), side) for m in range(2)]
        slots = [chip * 2 + c for chip in chips for c in range(2)]

        tokens_at(k, TOKENS[2 + layer])

        @pl.when(k < 2)
        def _():
            for chip in chips:
                for a in ((0, 2), (1, 3, 4, 5))[layer]:
                    tk(a, chip * 2 + 1 - core, None, 0, me, True).wait_recv()
            for s in slots:
                xn[s] = tg[layer, s].T

        def start(picks):
            def go():
                for m in picks:
                    sums(layer)[m].start()
            return go

        pl.when(k == 6)(lambda: add_far(layer))
        sources = [(ri.at[s, layer], rg.at[s, layer], tg.at[layer, s], xn.at[s], tg.at[2 + layer, s]) for s in slots]
        weight_part(e, wb.at[layer, e], sources, dwo.at[layer, n], ab, hid, dhs, dab, q)
        pl.when(k == 2)(start((0, 1)))
        pl.when(k == 4)(start((2,)))
        pl.when(k == 6)(start((3, 4, 5)))
        if not layer:
            pl.when(k == 4)(lambda: finish(1, tb_ref))
        return carry

    lax.fori_loop(0, 2 * side, functools.partial(weight_body, 1), 0)
    results = [put(0, xo_ref.at[0], xo_out), put(1, xo_ref.at[1], dxi_out), put(2, dgb_ref, dgb_out), put(3, dga_ref, dga_out)]
    for copy in results:
        copy.start()
    lax.fori_loop(0, 2 * side, functools.partial(weight_body, 0), 0)
    results.append(put(4, tb_ref, tb_out))
    results[-1].start()
    finish(0, ta_ref)
    results.append(put(5, ta_ref, ta_out))
    results[-1].start()
    for n, half in enumerate(ag_slots):
        view = wb.at[0, 0] if half is None else wb.at[0, 0, pl.ds(0, wh)]
        rdma(view, view, ag_send.at[n], ag_recv.at[0, 0, 0], me).wait_send()
    for a in range(6):
        for copy in tk_out(a) + tk_next(a) + tk_last(a):
            copy.wait_send()
    for layer in range(2):
        for copy in sums(layer):
            copy.wait_send()
    for copy in results:
        copy.wait()


def finish_kernel(xo_in, dxi_in, ta_in, tb_in, dga_in, dgb_in, xo_ref, dxi_ref, dw1a, dw3a, dw2a, dw1b, dw3b, dw2b, dga_ref, dgb_ref,
                  xo, dxi, ta, tb, dga, dgb, rows, dws, in_sem, out_sem):
    pairs = ((tb_in, tb), (xo_in, xo), (ta_in, ta), (dxi_in, dxi), (dga_in, dga), (dgb_in, dgb))
    loads = [pltpu.make_async_copy(src, dst, in_sem.at[n]) for n, (src, dst) in enumerate(pairs)]
    for copy in loads:
        copy.start()
    stores = []

    def put(src, dst):
        stores.append(pltpu.make_async_copy(src, dst, out_sem.at[len(stores)]))
        stores[-1].start()

    f = dw2a.shape[1]
    work = ((tb, dw1b, dw3b, dw2b, xo, xo_ref), (ta, dw1a, dw3a, dw2a, dxi, dxi_ref))
    for n, (total, dw1, dw3, dw2, cols, out) in enumerate(work):
        loads[2 * n].wait()
        put(total.at[pl.ds(2 * f, f)], dw2.at[0])
        for m, dw in enumerate((dw1, dw3)):
            dws[2 * n + m] = total[m * f : (m + 1) * f].T
        loads[2 * n + 1].wait()
        rows[n] = cols[...].T
        for m, dw in enumerate((dw1, dw3)):
            put(dws.at[2 * n + m], dw.at[0])
        loads[4 + n].wait()
        put((dga, dgb)[n], (dga_ref, dgb_ref)[n])
        put(rows.at[n], out)
    for copy in stores:
        copy.wait()


def solution(mesh):
    tok_spec = P(("dp", "ep"))
    w_spec = P("ep")
    members = mesh.shape["ep"]
    side = math.isqrt(members // 2)

    def device_program(x_in, idx_a, idx_b, gate_a, gate_b, dy_out, w1_a, w3_a, w2_a, w1_b, w3_b, w2_b):
        (tok, d), top, f = x_in.shape, idx_a.shape[1], w1_a.shape[2]
        any_ = pl.BlockSpec(memory_space=pl.ANY)
        two, row = 2, 2 * side
        shape = jax.ShapeDtypeStruct
        rows, dgs = shape((tok, d), BF16), shape((top, tok), F32)
        dws = (shape((1, d, f), F32), shape((1, d, f), F32), shape((1, f, d), F32))
        cols = shape((d, tok), BF16)
        wrows, grows = 2 * d + 2 * f, 3 * f
        outs = pl.pallas_call(
            functools.partial(step_kernel, side),
            out_shape=(cols, cols, shape((grows, d), F32), shape((grows, d), F32), dgs, dgs),
            in_specs=[any_] * 12,
            out_specs=(any_,) * 6,
            scratch_shapes=[
                *(pltpu.VMEM(dims, kind) for dims, kind in (
                    ((two, tok, d), BF16), ((two, d, tok), BF16), ((grows, d), F32), ((grows, d), F32), ((top, tok), F32), ((top, tok), F32),
                    ((two, members, wrows, f), BF16), ((side, row, d, tok), BF16), ((row, two, top, tok), jnp.int32), ((row, two, top, tok), F32),
                    ((row, tok, d), BF16), ((two, side, grows, d), F32), ((two, two, grows // two, d), F32), ((two, two, grows, d), F32),
                    ((d, tok), F32), ((d, tok), F32), ((side, two * f, tok), F32), ((side, f, tok), BF16), ((side, f, tok), F32),
                    ((side, two * f, tok), BF16), ((side, d, tok), BF16), ((two, d, tok), BF16), ((two, d, tok), BF16))),
                *(pltpu.SemaphoreType.DMA(dims) for dims in (
                    (row,), (row,), (row,), (80,), (two, members, two), (two, members), (row, row), (row, row, two), (row, row),
                    (two, row), (two, two), (two, side))),
            ],
            compiler_params=pltpu.CompilerParams(collective_id=0, has_side_effects=True, vmem_limit_bytes=56 * 2**20),
        )(x_in, dy_out, idx_a.T, idx_b.T, gate_a.T, gate_b.T, w1_a, w3_a, w2_a, w1_b, w3_b, w2_b)
        outs = pl.pallas_call(
            finish_kernel,
            out_shape=(rows, rows) + dws + dws + (dgs, dgs),
            in_specs=[any_] * 6,
            out_specs=(any_,) * 10,
            scratch_shapes=[
                pltpu.VMEM((d, tok), BF16),
                pltpu.VMEM((d, tok), BF16),
                pltpu.VMEM((grows, d), F32),
                pltpu.VMEM((grows, d), F32),
                pltpu.VMEM((top, tok), F32),
                pltpu.VMEM((top, tok), F32),
                pltpu.VMEM((two, tok, d), BF16),
                pltpu.VMEM((two * two, d, f), F32),
                pltpu.SemaphoreType.DMA((row,)),
                pltpu.SemaphoreType.DMA((two * row,)),
            ],
        )(*outs)
        return tuple(outs[:8]) + (outs[8].T, outs[9].T)

    return jax.shard_map(device_program, mesh=mesh, in_specs=(tok_spec,) * 6 + (w_spec,) * 6, out_specs=(tok_spec,) * 10, check_vma=False)
```

```python
import functools
import math

import jax
import jax.numpy as jnp
from jax import lax
from jax.experimental import pallas as pl
from jax.experimental.pallas import tpu as pltpu
from jax.sharding import PartitionSpec as P

F32 = jnp.float32
BF16 = jnp.bfloat16
MESH = pl.DeviceIdType.MESH

PLAN = {
    0: (100, 3, 30, 10, 1,),
    1: (210, 230,),
    2: (2, 110, 130,),
    4: (11, 13,),
    5: (20, 220, 120, 320,),
    6: (33, 31,),
    7: (12,),
    8: (23,),
    10: (21,),
    11: (123, 121, 32, 310, 330,),
    13: (22,),
    15: (122,),
    16: (111, 113,),
    17: (300,),
    18: (112, 133, 131,),
    20: (103, 101,),
    22: (132,),
    26: (102,),
}
SUMS = (
    {"far": 2, "near_up": 4, "near_down": 4, "join": 7, "line": 16, "last": 30},
    {"far": 2, "near_up": 4, "near_down": 4, "join": 7, "line": 13, "last": 29},
)


def mm(a, b, ca, cb):
    return lax.dot_general(a, b, (((ca,), (cb,)), ((), ())), preferred_element_type=F32)


def route(expert, idx_t, gate_t):
    picked = idx_t == expert
    gate = jnp.sum(jnp.where(picked, gate_t, 0.0), axis=0, keepdims=True)
    count = jnp.sum(jnp.where(picked, 1.0, 0.0), axis=0, keepdims=True)
    return picked, gate, count > 0.5


def up_rows(w, d):
    return jnp.concatenate([w[pl.ds(0, d)], w[pl.ds(d, d)]], axis=1)


def down_rows(w, d):
    return jnp.concatenate([w[pl.ds(2 * d, d // 2)], w[pl.ds(2 * d + d // 2, d // 2)]], axis=1)


def strips(rows):
    return [pl.ds(row, 16) for row in range(0, rows, 16)]


def forward_pair(experts, idx_t, gate_t, x_t, acc, ab, hid, o16):
    d, f = x_t.shape[0], hid.shape[1]
    gates = []
    for n, (e, w) in enumerate(experts):
        _, gate, mask = route(e, idx_t, gate_t)
        gates.append(gate)
        ab[n] = jnp.where(mask, mm(up_rows(w, d), x_t[...], 0, 0), 0.0)
    for n, (e, w) in enumerate(experts):
        for row in range(0, f, 16):
            u = ab[n, row : row + 16]
            hid[n, row : row + 16] = (u * jax.nn.sigmoid(u) * ab[n, f + row : f + row + 16]).astype(BF16)
        o16[n] = mm(down_rows(w, d), hid[n], 0, 0).astype(BF16)
    for part in strips(d):
        acc[part] += gates[0] * o16[0, part].astype(F32) + gates[1] * o16[1, part].astype(F32)


def backward_pair(experts, idx_t, gate_t, x_t, x, dy_t, acc, dxs, dg, ab, hid, dhs, dab, q, o16, du16):
    d, f = x_t.shape[0], hid.shape[1]
    gates, picks = [], []
    for n, (e, w, _) in enumerate(experts):
        picked, gate, mask = route(e, idx_t, gate_t)
        gates.append(gate)
        picks.append(picked)
        for part in strips(d):
            q[n, part] = (gate * dy_t[part].astype(F32)).astype(BF16)
        ab[n] = jnp.where(mask, mm(up_rows(w, d), x_t[...], 0, 0), 0.0)
        dhs[n] = mm(down_rows(w, d), q[n], 1, 0)
    for n, (e, w, dst) in enumerate(experts):
        for row in range(0, f, 16):
            u, v = ab[n, row : row + 16], ab[n, f + row : f + row + 16]
            dh = dhs[n, row : row + 16]
            s = jax.nn.sigmoid(u)
            silu = u * s
            hid[n, row : row + 16] = (silu * v).astype(BF16)
            dab[n, row : row + 16] = (dh * v * (s + silu * (1.0 - s))).astype(BF16)
            dab[n, f + row : f + row + 16] = (dh * silu).astype(BF16)
        o16[n] = mm(down_rows(w, d), hid[n], 0, 0).astype(BF16)
        du16[n] = mm(up_rows(w, d), dab[n], 1, 0).astype(BF16)
        dst[: 2 * f] = mm(dab[n], x[...], 1, 0)
        dst[2 * f :] = mm(hid[n], q[n], 1, 1)
    sums = [0.0, 0.0]
    for part in strips(d):
        dy = dy_t[part].astype(F32)
        outs = [o16[n, part].astype(F32) for n in range(2)]
        if acc is not None:
            acc[part] += gates[0] * outs[0] + gates[1] * outs[1]
        for n in range(2):
            prod = dy * outs[n]
            sums[n] = sums[n] + (prod[:8] + prod[8:])
        dxs[part] += du16[0, part].astype(F32) + du16[1, part].astype(F32)
    dg[...] += jnp.where(picks[0], jnp.sum(sums[0], axis=0, keepdims=True), 0.0) + jnp.where(picks[1], jnp.sum(sums[1], axis=0, keepdims=True), 0.0)


def near_order(g):
    return g + lax.div(g, 2) * (1 - 2 * lax.rem(g, 2))


def far_order(g):
    return 2 - g + lax.div(g, 2) * (3 - 2 * lax.rem(g, 2))


def step_kernel(side, x_in, dy_in, ia_in, ib_in, ga_in, gb_in, w1a, w3a, w2a, w1b, w3b, w2b,
                xo_out, dxi_out, ta_out, tb_out, dga_out, dgb_out,
                x_ref, dy_ref, ia_ref, ib_ref, ga_ref, gb_ref, xo_ref, ta_ref, tb_ref, dga_ref, dgb_ref, in_sem, out_sem, wb, dwo, dws, rb, ah, af, bh, bf, xt, xm, xmt, dyt, acc, dxs, ab, hid, dhs, dab, q, o16, du16,
                load_sem, ag_send, ag_recv, ag_pair, d_send, d_recv, pa_send, ah_recv, af_recv, pb_send, bh_recv, bf_recv):
    me = lax.axis_index("ep")
    core, chip = lax.rem(me, 2), lax.div(me, 2)
    cx, cy = lax.rem(chip, side), lax.div(chip, side)
    p = cx * (1 - core) + cy * core
    r = cy * (1 - core) + cx * core
    tok, d = x_ref.shape
    f = w1a.shape[2]
    wrows, grows = wb.shape[2], dwo.shape[2]
    wh, gh = wrows // 2, grows // 2
    steps = side * side
    ring = dws.shape[0]

    def member(i, j, c):
        return ((j * (1 - c) + i * c) * side + i * (1 - c) + j * c) * 2 + c

    def at(di, dj):
        return member(lax.rem(p + di, side), lax.rem(r + dj, side), core)

    sib = me + 1 - 2 * core
    first = {1: at(1, 0), -1: at(side - 1, 0)}
    second = {1: at(0, 1), -1: at(0, side - 1)}

    def rdma(src, dst, send, recv, dev):
        return pltpu.make_async_remote_copy(src_ref=src, dst_ref=dst, send_sem=send, recv_sem=recv, device_id={"ep": dev}, device_id_type=MESH)

    loads = []
    for layer, (w1, w3, w2) in enumerate(((w1a, w3a, w2a), (w1b, w3b, w2b))):
        parts = (w1.at[0], w3.at[0], w2.at[0, :, pl.ds(0, d // 2)], w2.at[0, :, pl.ds(d // 2, d // 2)])
        row = 0
        for n, part in enumerate(parts):
            loads.append(pltpu.make_async_copy(part, wb.at[layer, me, pl.ds(row, part.shape[0])], load_sem.at[4 * layer + n]))
            row += part.shape[0]
    for copy in loads:
        copy.start()

    barrier = pltpu.get_barrier_semaphore()
    tokens = [pltpu.make_async_copy(src, dst, in_sem.at[n]) for n, (src, dst) in enumerate((
        (x_in, x_ref), (ia_in, ia_ref), (ga_in, ga_ref), (dy_in, dy_ref), (ib_in, ib_ref), (gb_in, gb_ref)))]

    def put(n, src, dst):
        return pltpu.make_async_copy(src, dst, out_sem.at[n])

    for dev in (sib, *first.values(), *second.values()):
        pl.semaphore_signal(barrier, inc=1, device_id={"ep": dev}, device_id_type=MESH)
    for copy in tokens:
        copy.start()
    pl.semaphore_wait(barrier, 5)

    ag_slots = []

    def ag_copy(layer, e, half, dev, pair=False):
        view = wb.at[layer, e] if half is None else wb.at[layer, e, pl.ds(half * wh, wh)]
        recv = ag_pair.at[layer, e] if pair else ag_recv.at[layer, e, half or 0]
        copy = rdma(view, view, ag_send.at[len(ag_slots)], recv, dev)
        ag_slots.append(half)
        copy.start()

    def ag_wait(layer, e, half):
        view = wb.at[layer, e] if half is None else wb.at[layer, e, pl.ds(half * wh, wh)]
        rdma(view, view, ag_send.at[0], ag_recv.at[layer, e, half or 0], me).wait_recv()

    def spread(layer, di):
        for dev in second.values():
            ag_copy(layer, at(di, 0), None, dev)

    def arrive(layer, di, dj):
        e = at(di, dj)
        last = dj or di
        if last == 2:
            ag_wait(layer, e, 0)
            ag_wait(layer, e, 1)
        elif last:
            ag_wait(layer, e, None)
        line = second if dj else first
        if last == 3:
            ag_copy(layer, e, 0, line[1])
        if last == 1:
            ag_copy(layer, e, 1, line[-1])
        ag_copy(layer, e, None, sib, pair=True)

    def own_out(layer):
        for dev in first.values():
            ag_copy(layer, me, None, dev)

    def pair_wait(layer, e):
        view = wb.at[layer, e]
        rdma(view, view, ag_send.at[0], ag_pair.at[layer, e], me).wait_recv()

    for copy in loads[:4]:
        copy.wait()
    own_out(0)
    arrive(0, 0, 0)
    spread(0, 0)
    for copy in tokens:
        copy.wait()
    xt[...] = x_ref[...].T
    dyt[...] = dy_ref[...].T
    acc[...] = xt[...].astype(F32)
    dxs[...] = dyt[...].astype(F32)
    dga_ref[...] = jnp.zeros_like(dga_ref)
    dgb_ref[...] = jnp.zeros_like(dgb_ref)
    for copy in loads[4:]:
        copy.wait()

    def moves_at(k, base):
        for step in range(steps):
            todo = PLAN.get(base + step)
            if todo:
                @pl.when(k == step)
                def _():
                    for code in todo:
                        kind, block = divmod(code, 100)
                        kind, layer = divmod(kind, 2)
                        di, dj = divmod(block, 10)
                        if kind == 1:
                            spread(layer, di)
                        else:
                            if not block:
                                own_out(layer)
                            arrive(layer, di, dj)

    def pick(order, k):
        a, b = order(lax.div(k, side)), order(lax.rem(k, side))
        return at(a, b), member(lax.rem(r + a, side), lax.rem(p + b, side), 1 - core)

    def forward_body(k, carry):
        moves_at(k, 0)
        own, other = pick(near_order, k)
        pair_wait(0, other)
        forward_pair([(e, wb.at[0, e]) for e in (own, other)], ia_ref[...], ga_ref[...], xt, acc, ab, hid, o16)
        return carry

    lax.fori_loop(0, steps, forward_body, 0)
    xmt[...] = acc[...].astype(BF16)
    xm[...] = xmt[...].T
    acc[...] = xmt[...].astype(F32)

    def pair_send(layer, k):
        slot = lax.rem(k, ring)
        return rdma(dws.at[slot], rb.at[layer, k], d_send.at[slot], d_recv.at[layer, k], sib)

    def join(layer, k):
        pair_send(layer, k).wait_recv()
        dwo[layer, k] += rb[layer, k]

    lo, hi = pl.ds(0, gh), pl.ds(gh, gh)

    def far_copies(layer, g):
        return (rdma(dwo.at[layer, 4 * g, lo], ah.at[layer, g, 0], pa_send.at[layer, g, 0], ah_recv.at[layer, g, 0], second[1]),
                rdma(dwo.at[layer, 4 * g, hi], ah.at[layer, g, 1], pa_send.at[layer, g, 1], ah_recv.at[layer, g, 1], second[-1]))

    def near_copies(layer, g):
        up, down = dwo.at[layer, 4 * g + 1], dwo.at[layer, 4 * g + 2]
        up_in, down_in = af.at[layer, g, 0], af.at[layer, g, 1]
        return tuple(
            rdma(src.at[part], dst.at[part], pa_send.at[layer, g, 2 + n], af_recv.at[layer, g, n], dev)
            for n, (src, dst, part, dev) in enumerate((
                (up, up_in, hi, second[1]), (up, up_in, lo, second[1]),
                (down, down_in, lo, second[-1]), (down, down_in, hi, second[-1]))))

    def line_far(layer):
        return (rdma(dwo.at[layer, 3, lo], bh.at[layer, 0], pb_send.at[layer, 0], bh_recv.at[layer, 0], first[1]),
                rdma(dwo.at[layer, 3, hi], bh.at[layer, 1], pb_send.at[layer, 1], bh_recv.at[layer, 1], first[-1]))

    def line_near(layer):
        return (rdma(dwo.at[layer, 7], bf.at[layer, 0], pb_send.at[layer, 2], bf_recv.at[layer, 0], first[1]),
                rdma(dwo.at[layer, 11], bf.at[layer, 1], pb_send.at[layer, 3], bf_recv.at[layer, 1], first[-1]))

    def add_far(layer, g):
        for n, copy in enumerate(far_copies(layer, g)):
            copy.wait_recv()
            part = pl.ds(n * gh, gh)
            dwo[layer, 4 * g + 1 + n, part] += ah[layer, g, n]

    def add_near(layer, g):
        for copy in near_copies(layer, g):
            copy.wait_recv()
        dwo[layer, 4 * g + 3] += af[layer, g, 0] + af[layer, g, 1]

    def add_line(layer, n):
        line_far(layer)[n].wait_recv()
        part = pl.ds(n * gh, gh)
        dwo[layer, 7 + 4 * n, part] += bh[layer, n]

    def finish(layer, out):
        add_near(layer, 3)
        for copy in line_near(layer):
            copy.wait_recv()
        out[...] = dwo[layer, 15] + bf[layer, 0] + bf[layer, 1]

    def when(cond, fn):
        if isinstance(cond, bool):
            if cond:
                fn()
        else:
            pl.when(cond)(fn)

    def each_group(kk, off, groups, fn):
        if isinstance(kk, int):
            if kk >= off and (kk - off) % 4 == 0 and (kk - off) // 4 < groups:
                fn((kk - off) // 4)
        else:
            pl.when((kk >= off) & (lax.rem(kk - off + 32, 4) == 0) & (kk < off + 4 * groups))(lambda: fn(lax.div(kk - off, 4)))

    def later(kk, first_step, last_step):
        return isinstance(kk, int) or (first_step < steps if kk is sweep[0] else last_step >= steps)

    def middle(layer, kk):
        at_ = SUMS[layer]
        if later(kk, at_["join"], at_["join"] + 12):
            each_group(kk, at_["join"], 4, functools.partial(add_far, layer))
        if later(kk, at_["line"], at_["line"] + 8):
            each_group(kk, at_["line"], 3, functools.partial(add_near, layer))
            when(kk == at_["line"] + 4, lambda: add_line(layer, 0))
            when(kk == at_["line"] + 8, lambda: add_line(layer, 1))
        if later(kk, at_["last"], at_["last"]):
            when(kk == at_["last"], lambda: finish(layer, (ta_ref, tb_ref)[layer]))

    def end(layer, kk):
        at_ = SUMS[layer]

        def start(copies, picks):
            def go(*g):
                made = copies(layer, *g)
                for n in picks:
                    made[n].start()
            return go

        for key, copies, picks in (("far", far_copies, (0, 1)), ("near_up", near_copies, (0,)), ("near_down", near_copies, (2,)), ("join", near_copies, (1, 3))):
            if later(kk, at_[key], at_[key] + 12):
                each_group(kk, at_[key], 4, start(copies, picks))
        if later(kk, at_["line"], at_["line"] + 8):
            when(kk == at_["line"], start(line_far, (0, 1)))
            when(kk == at_["line"] + 4, start(line_near, (0,)))
            when(kk == at_["line"] + 8, start(line_near, (1,)))

    sweep = [None]

    def backward_body(layer, k, carry):
        sweep[0] = k
        own, other = pick(far_order, k)
        if layer:
            moves_at(k, steps)
            pair_wait(1, other)

            @pl.when(k >= ring)
            def _():
                pair_send(layer, k).wait_send()
        else:
            pair_send(layer, k).wait_send()
            pl.when(k < 2)(lambda: join(1, k + steps - 2))
            middle(1, k + steps)
        pl.when(k >= 2)(lambda: join(layer, k - 2))
        middle(layer, k)
        experts = [(other, wb.at[layer, other], dws.at[lax.rem(k, ring)]), (own, wb.at[layer, own], dwo.at[layer, k])]
        idx, gates, dg, feat, rows = ((ia_ref, ga_ref, dga_ref, xt, x_ref), (ib_ref, gb_ref, dgb_ref, xmt, xm))[layer]
        backward_pair(experts, idx[...], gates[...], feat, rows, dyt, acc if layer else None, dxs, dg, ab, hid, dhs, dab, q, o16, du16)
        if not layer:
            end(1, k + steps)
        end(layer, k)
        pair_send(layer, k).start()
        return carry

    lax.fori_loop(0, steps, functools.partial(backward_body, 1), 0)
    dyt[...] = dxs[...].astype(BF16)
    dxs[...] = dyt[...].astype(F32)
    xo_ref[...] = acc[...].astype(BF16)
    lax.fori_loop(0, steps, functools.partial(backward_body, 0), 0)
    results = [put(0, xo_ref, xo_out), put(1, tb_ref, tb_out), put(2, dgb_ref, dgb_out)]
    dyt[...] = dxs[...].astype(BF16)
    results += [put(3, dyt, dxi_out), put(4, dga_ref, dga_out)]
    for kk in range(steps, SUMS[0]["last"] + 1):
        if kk < steps + 2:
            join(0, kk - 2)
        middle(0, kk)
        end(0, kk)
        if kk == steps + 1:
            for copy in results:
                copy.start()

    results.append(put(5, ta_ref, ta_out))
    results[-1].start()
    for n, half in enumerate(ag_slots):
        view = wb.at[0, 0] if half is None else wb.at[0, 0, pl.ds(0, wh)]
        rdma(view, view, ag_send.at[n], ag_recv.at[0, 0, 0], me).wait_send()
    for k in range(steps - ring, steps):
        pair_send(0, k).wait_send()
    for layer in range(2):
        for g in range(side):
            for copy in far_copies(layer, g) + near_copies(layer, g):
                copy.wait_send()
        for copy in line_far(layer) + line_near(layer):
            copy.wait_send()
    for copy in results:
        copy.wait()


def finish_kernel(xo_in, dxi_in, ta_in, tb_in, dga_in, dgb_in, xo_ref, dxi_ref, dw1a, dw3a, dw2a, dw1b, dw3b, dw2b, dga_ref, dgb_ref,
                  xo, dxi, ta, tb, dga, dgb, rows, dws, in_sem, out_sem):
    pairs = ((tb_in, tb), (xo_in, xo), (ta_in, ta), (dxi_in, dxi), (dga_in, dga), (dgb_in, dgb))
    loads = [pltpu.make_async_copy(src, dst, in_sem.at[n]) for n, (src, dst) in enumerate(pairs)]
    for copy in loads:
        copy.start()
    stores = []

    def put(src, dst):
        stores.append(pltpu.make_async_copy(src, dst, out_sem.at[len(stores)]))
        stores[-1].start()

    f = dw2a.shape[1]
    work = ((tb, dw1b, dw3b, dw2b, xo, xo_ref), (ta, dw1a, dw3a, dw2a, dxi, dxi_ref))
    for n, (total, dw1, dw3, dw2, cols, out) in enumerate(work):
        loads[2 * n].wait()
        put(total.at[pl.ds(2 * f, f)], dw2.at[0])
        for m, dw in enumerate((dw1, dw3)):
            dws[2 * n + m] = total[m * f : (m + 1) * f].T
        loads[2 * n + 1].wait()
        rows[n] = cols[...].T
        for m, dw in enumerate((dw1, dw3)):
            put(dws.at[2 * n + m], dw.at[0])
        loads[4 + n].wait()
        put((dga, dgb)[n], (dga_ref, dgb_ref)[n])
        put(rows.at[n], out)
    for copy in stores:
        copy.wait()


def solution(mesh):
    tok_spec = P(("dp", "ep"))
    w_spec = P("ep")
    members = mesh.shape["ep"]
    side = math.isqrt(members // 2)
    chips = side * side

    def device_program(x_in, idx_a, idx_b, gate_a, gate_b, dy_out, w1_a, w3_a, w2_a, w1_b, w3_b, w2_b):
        (tok, d), top, f = x_in.shape, idx_a.shape[1], w1_a.shape[2]
        any_ = pl.BlockSpec(memory_space=pl.ANY)
        shape = jax.ShapeDtypeStruct
        rows, dgs = shape((tok, d), BF16), shape((top, tok), F32)
        dws = (shape((1, d, f), F32), shape((1, d, f), F32), shape((1, f, d), F32))
        cols = shape((d, tok), BF16)
        wrows, grows = 2 * d + 2 * f, 3 * f
        outs = pl.pallas_call(
            functools.partial(step_kernel, side),
            out_shape=(cols, cols, shape((grows, d), F32), shape((grows, d), F32), dgs, dgs),
            in_specs=[any_] * 12,
            out_specs=(any_,) * 6,
            scratch_shapes=[
                pltpu.VMEM((tok, d), BF16),
                pltpu.VMEM((tok, d), BF16),
                pltpu.VMEM((top, tok), jnp.int32),
                pltpu.VMEM((top, tok), jnp.int32),
                pltpu.VMEM((top, tok), F32),
                pltpu.VMEM((top, tok), F32),
                pltpu.VMEM((d, tok), BF16),
                pltpu.VMEM((grows, d), F32),
                pltpu.VMEM((grows, d), F32),
                pltpu.VMEM((top, tok), F32),
                pltpu.VMEM((top, tok), F32),
                pltpu.SemaphoreType.DMA((6,)),
                pltpu.SemaphoreType.DMA((6,)),
                pltpu.VMEM((2, members, wrows, f), BF16),
                pltpu.VMEM((2, chips, grows, d), F32),
                pltpu.VMEM((4, grows, d), F32),
                pltpu.VMEM((2, chips, grows, d), F32),
                pltpu.VMEM((2, side, 2, grows // 2, d), F32),
                pltpu.VMEM((2, side, 2, grows, d), F32),
                pltpu.VMEM((2, 2, grows // 2, d), F32),
                pltpu.VMEM((2, 2, grows, d), F32),
                pltpu.VMEM((d, tok), BF16),
                pltpu.VMEM((tok, d), BF16),
                pltpu.VMEM((d, tok), BF16),
                pltpu.VMEM((d, tok), BF16),
                pltpu.VMEM((d, tok), F32),
                pltpu.VMEM((d, tok), F32),
                pltpu.VMEM((2, 2 * f, tok), F32),
                pltpu.VMEM((2, f, tok), BF16),
                pltpu.VMEM((2, f, tok), F32),
                pltpu.VMEM((2, 2 * f, tok), BF16),
                pltpu.VMEM((2, d, tok), BF16),
                pltpu.VMEM((2, d, tok), BF16),
                pltpu.VMEM((2, d, tok), BF16),
                pltpu.SemaphoreType.DMA((8,)),
                pltpu.SemaphoreType.DMA((72,)),
                pltpu.SemaphoreType.DMA((2, members, 2)),
                pltpu.SemaphoreType.DMA((2, members)),
                pltpu.SemaphoreType.DMA((4,)),
                pltpu.SemaphoreType.DMA((2, chips)),
                pltpu.SemaphoreType.DMA((2, side, 6)),
                pltpu.SemaphoreType.DMA((2, side, 2)),
                pltpu.SemaphoreType.DMA((2, side, 4)),
                pltpu.SemaphoreType.DMA((2, 4)),
                pltpu.SemaphoreType.DMA((2, 2)),
                pltpu.SemaphoreType.DMA((2, 2)),
            ],
            compiler_params=pltpu.CompilerParams(collective_id=0, has_side_effects=True, vmem_limit_bytes=62 * 2**20),
        )(x_in, dy_out, idx_a.T, idx_b.T, gate_a.T, gate_b.T, w1_a, w3_a, w2_a, w1_b, w3_b, w2_b)
        outs = pl.pallas_call(
            finish_kernel,
            out_shape=(rows, rows) + dws + dws + (dgs, dgs),
            in_specs=[any_] * 6,
            out_specs=(any_,) * 10,
            scratch_shapes=[
                pltpu.VMEM((d, tok), BF16),
                pltpu.VMEM((d, tok), BF16),
                pltpu.VMEM((grows, d), F32),
                pltpu.VMEM((grows, d), F32),
                pltpu.VMEM((top, tok), F32),
                pltpu.VMEM((top, tok), F32),
                pltpu.VMEM((2, tok, d), BF16),
                pltpu.VMEM((4, d, f), F32),
                pltpu.SemaphoreType.DMA((6,)),
                pltpu.SemaphoreType.DMA((10,)),
            ],
        )(*outs)
        return tuple(outs[:8]) + (outs[8].T, outs[9].T)

    return jax.shard_map(device_program, mesh=mesh, in_specs=(tok_spec,) * 6 + (w_spec,) * 6, out_specs=(tok_spec,) * 10, check_vma=False)
```
